256 devices in a mesh: dp: 8 (over y, core), seq: 32 (over x, z).
Axes of the slice: x: 4, y: 4, z: 8, core: 2. Of those that a mesh axis runs over, the one named last changes fastest.
Arguments:
- tokens: bfloat16 [262144, 2048], P(('dp', 'seq')), parts along dimension 0, may hold values from -6 to 6
- chosen: int32 [32768], P('dp'), parts along dimension 0, may hold values from 0 to 32767, as said below
- gates: float32 [32768], P('dp'), parts along dimension 0, may hold values from 0.5 to 2
- w_query: bfloat16 [2048, 1024], P('seq'), may hold values from -1.8561553 to 1.8561553
- w_key: bfloat16 [2048, 256], P('seq'), may hold values from -0.088388348 to 0.088388348
- w_value: bfloat16 [2048, 256], P('seq'), may hold values from -0.125 to 0.125
- w_out: bfloat16 [1024, 2048], P(None, 'seq'), may hold values from -0.5 to 0.5
Outputs:
- mixed: bfloat16 [262144, 2048], P(('dp', 'seq')), parts along dimension 0
The draws below stay inside these ranges and needn't reach their ends.
There are 8 independent parts, one for each index of `dp`. The reference program is written for one: setup_inputs(seed, part) draws one part's arguments, and reference() takes and returns one part's arrays. A program takes and returns all parts, laid end to end along the dimension named above; an argument that names none is the same for every part. Nothing has to cross between parts.
Inputs may be any that keep to these rules, and one draw needn't show every extreme that they name: `chosen`: distinct positions in increasing order; at most 256 of them lie in one device's 1024 consecutive positions, and exactly 256 lie in some device's positions.
All inputs are finite; a program needn't handle non-finite values.
Results may differ from the reference program's by a relative error of at most 0.006.
Values may be sent and summed in bfloat16 or wider, within the bound.
A program may use at most 128 MiB of HBM per device.

```python
import math
import jax
import jax.numpy as jnp
from jax import lax

D = 2048
HEADS = 8
KV_HEADS = 2
HEAD_DIM = 128
TOK_DEV = 1024
ROWS_DEV = 128
TOKENS = 32768
CHOSEN = 4096
N_SEQ = 32


def draw_chosen(key, part):
    lifts = jax.random.randint(jax.random.fold_in(key, 1), (N_SEQ,), 0, ROWS_DEV + 1)
    heavy = jax.random.randint(jax.random.fold_in(key, 2), (), 0, N_SEQ)
    order = jnp.arange(N_SEQ, dtype=jnp.int32)
    lifts = jnp.where(order == heavy, ROWS_DEV, lifts)
    lifts = jnp.where(order == (heavy + N_SEQ - 1) % N_SEQ, 0, lifts)
    counts = ROWS_DEV + lifts - jnp.roll(lifts, 1)
    subkeys = jax.random.split(jax.random.fold_in(key, 3), N_SEQ)
    ranks = jax.vmap(lambda single: jax.random.permutation(single, TOK_DEV))(subkeys)
    flags = (ranks < counts[:, None]).reshape(-1)
    return jnp.nonzero(flags, size=CHOSEN)[0].astype(jnp.int32)


def shared_base(key):
    raw = jax.random.normal(jax.random.fold_in(key, 11), (D, KV_HEADS * HEAD_DIM), jnp.float32)
    return jnp.clip(raw, -4.0, 4.0) * D ** (-0.5)


def draw_w_key(key, part):
    return shared_base(key).astype(jnp.bfloat16)


def draw_w_query(key, part):
    raw = jax.random.normal(jax.random.fold_in(key, 12), (D, HEADS * HEAD_DIM), jnp.float32)
    noise = jnp.clip(raw, -4.0, 4.0) * 2.0 * D ** (-0.5)
    return noise.astype(jnp.bfloat16)


def steps_of(rng, dims, cuts, least, top_value):
    gain = 1.0
    for position, shards_of in cuts:
        steps = jax.random.uniform(jax.random.fold_in(jax.random.fold_in(rng, 6), position), (shards_of,), jnp.float32, least / len(cuts), top_value / len(cuts))
        gain = gain * jnp.repeat(jnp.exp(steps), dims[position] // shards_of).reshape((-1,) + (1,) * (len(dims) - 1 - position))
    return gain


def bell_draw(rng, dims, spread, limit, cuts=(), kind=jnp.bfloat16):
    drawn = spread * jax.random.normal(rng, dims, jnp.float32)
    if cuts:
        drawn = drawn * steps_of(rng, dims, cuts, -0.22, 0.18)
    return jnp.clip(drawn, -limit, limit).astype(kind)


def setup_inputs(seed: int = 0, part: int = 0) -> dict:
    splits = jax.random.split(jax.random.key(seed), 8)
    part_splits = jax.random.split(jax.random.fold_in(splits[7], part), 8)
    return {
        "tokens": bell_draw(part_splits[0], (TOKENS, D), 1.0, 6.0, ((0, 32),)),
        "chosen": draw_chosen(jax.random.fold_in(jax.random.fold_in(splits[7], part), 71), part),
        "gates": jnp.clip(jax.random.uniform(part_splits[2], (CHOSEN,), jnp.float32, 0.5, 2.0), 0.5, 2.0),
        "w_query": draw_w_query(jax.random.fold_in(splits[7], 71), part),
        "w_key": draw_w_key(jax.random.fold_in(splits[7], 71), part),
        "w_value": bell_draw(splits[5], (D, KV_HEADS * HEAD_DIM), D ** -0.5, 0.125, ((0, 32),)),
        "w_out": bell_draw(splits[6], (HEADS * HEAD_DIM, D), (HEADS * HEAD_DIM // 9) ** -0.5, 0.5, ((1, 32),)),
    }


neg_fill = -1e+30

def reference(tokens, chosen, gates, w_query, w_key, w_value, w_out):
    picked_total = chosen.shape[0]
    group_size = HEADS // KV_HEADS
    block_rows = math.gcd(picked_total, 512)
    picked = tokens[chosen].astype(jnp.float32)
    normed = (picked * lax.rsqrt(lax.optimization_barrier(jnp.mean(picked * picked, axis=1, keepdims=True)) + 1e-06)).astype(jnp.bfloat16)
    query_matrix = (jnp.dot(normed, w_query, preferred_element_type=jnp.float32) * HEAD_DIM ** (-0.5)).astype(jnp.bfloat16)
    keys_all = jnp.dot(normed, w_key, preferred_element_type=jnp.float32).astype(jnp.bfloat16)
    values = jnp.dot(normed, w_value, preferred_element_type=jnp.float32).astype(jnp.bfloat16)
    query_matrix = lax.optimization_barrier(query_matrix).astype(jnp.float32)
    keys_expanded = lax.optimization_barrier(keys_all).astype(jnp.float32).reshape(picked_total, KV_HEADS, HEAD_DIM)
    values_expanded = lax.optimization_barrier(values).astype(jnp.float32).reshape(picked_total, KV_HEADS, HEAD_DIM)
    blocks = query_matrix.reshape(picked_total // block_rows, block_rows, KV_HEADS, group_size, HEAD_DIM)
    firsts = (jnp.arange(picked_total // block_rows, dtype=jnp.int32) * block_rows).astype(jnp.int32)
    key_order = jnp.arange(picked_total, dtype=jnp.int32)

    def one_block(inputs):
        query_tile, first_row = inputs
        logit_scores = jnp.einsum('qjfh,ujh->jfqu', query_tile, keys_expanded)
        query_order = first_row + jnp.arange(block_rows, dtype=jnp.int32)
        allowed = key_order[None, :] <= query_order[:, None]
        logit_scores = jnp.where(allowed, logit_scores, neg_fill)
        top_score = lax.optimization_barrier(jnp.max(logit_scores, axis=-1, keepdims=True))
        probs = jnp.where(allowed, jnp.exp(logit_scores - top_score), 0.0)
        totals = lax.optimization_barrier(jnp.sum(probs, axis=-1))
        softmax_weights = lax.optimization_barrier(probs.astype(jnp.bfloat16)).astype(jnp.float32)
        summed_total = jnp.einsum('yoih,hyf->yoif', softmax_weights, values_expanded)
        attended = summed_total / totals[..., None]
        return jnp.transpose(attended, (2, 0, 1, 3)).reshape(block_rows, HEADS * HEAD_DIM)
    attended = lax.map(one_block, (blocks, firsts)).reshape(picked_total, HEADS * HEAD_DIM).astype(jnp.bfloat16)
    block_out = jnp.dot(attended, w_out, preferred_element_type=jnp.float32).astype(jnp.bfloat16)
    block_wide = lax.optimization_barrier(block_out).astype(jnp.float32)
    mixed = tokens.astype(jnp.float32).at[chosen].add(gates[:, None] * block_wide)
    return mixed.astype(jnp.bfloat16)
```

```python
import functools

import jax
import jax.numpy as jnp
from jax import lax
from jax.experimental import pallas as pl
from jax.experimental.pallas import tpu as pltpu
from jax.sharding import PartitionSpec as P

HEADS = 8
KV_HEADS = 2
GROUP = HEADS // KV_HEADS
HEAD_DIM = 128
D = 2048
QW = HEADS * HEAD_DIM
KW = KV_HEADS * HEAD_DIM
W = QW + 2 * KW
SEQ = 32
NX = 4
NZ = 8
TOK = 1024
CHOSEN = 4096
ROWS = 128
MOST = 256
SLOTS = 8
DEPTH = D // SEQ
HALF = DEPTH // 2
MESH = pl.DeviceIdType.MESH
F32 = jnp.float32
BF16 = jnp.bfloat16
FAR = -1e30


def ring_steps(a, b, na, nb, index_of, start, wait, arrived):
    def node(da, db):
        return index_of(lax.rem(a + da + na, na), lax.rem(b + db + nb, nb))

    def reach(order, n):
        return (n // 2, n // 2 - 1) if order % 2 == 0 else (n // 2 - 1, n // 2)

    def first():
        own = node(0, 0)
        for da, db in ((1, 0), (-1, 0), (0, 1), (0, -1)):
            start(own, node(da, db))

    def along_a(k, side):
        block = node(-side * k, 0)
        wait(block)
        limit = na // 2 if side == 1 else na // 2 - 1
        if k < limit:
            start(block, node(side, 0))
        start(block, node(0, 1))
        start(block, node(0, -1))
        arrived(block)

    def along_b(order, j, m, side):
        block = node(j, -side * m)
        wait(block)
        limit = reach(order, nb)[0 if side == 1 else 1]
        if m < limit:
            start(block, node(0, side))
        arrived(block)

    steps = [first]
    columns = [0]
    for k in range(1, na // 2 + 1):
        steps.append(functools.partial(along_a, k, 1))
        columns.append(-k)
        if k < na // 2:
            steps.append(functools.partial(along_a, k, -1))
            columns.append(k)
    for m in range(1, nb // 2 + 1):
        for order, j in enumerate(columns):
            plus, minus = reach(order, nb)
            if m <= plus:
                steps.append(functools.partial(along_b, order, j, m, 1))
            if m <= minus:
                steps.append(functools.partial(along_b, order, j, m, -1))
    return steps


def block_kernel(
    tokens, wq, wk, wv, wo, crow, grow, c2, c2t,
    out, meta,
    tok, weights, wots, wo_in, normed, onehot, bias, query, att, kv_slots, kv_in, kv,
    cpos, bar_unused, load_sem, tok_sem, ici_send, w_recv, o_recv, kv_recv, a_send, a_recv,
    d2d_send, d2d_recv,
):
    dp = lax.axis_index("dp")
    me = lax.axis_index("seq")
    core = lax.rem(dp, 2)
    partner = dp + 1 - 2 * core
    x, z = me // NZ, lax.rem(me, NZ)

    w_rows = pl.ds(pl.multiple_of(me * DEPTH, DEPTH), DEPTH)
    loads = [
        pltpu.make_async_copy(wq, weights.at[w_rows, 0:QW], load_sem.at[0]),
        pltpu.make_async_copy(wk, weights.at[w_rows, QW : QW + KW], load_sem.at[1]),
        pltpu.make_async_copy(wv, weights.at[w_rows, QW + KW : W], load_sem.at[2]),
        pltpu.make_async_copy(wo, wo_in, load_sem.at[3]),
    ]
    for copy in loads:
        copy.start()
    token_load = pltpu.make_async_copy(tokens, tok, tok_sem)
    token_load.start()

    barrier = pltpu.get_barrier_semaphore()

    def greet(j, carry):
        pl.semaphore_signal(
            barrier, inc=1, device_id=(dp, lax.rem(me + j, SEQ)), device_id_type=MESH
        )
        return carry

    lax.fori_loop(1, SEQ, greet, 0)
    pl.semaphore_signal(barrier, inc=1, device_id=(partner, me), device_id_type=MESH)
    pl.semaphore_wait(barrier, SEQ)

    def gather(view, recv, stage, shared):
        def ici(block, dest):
            return pltpu.make_async_remote_copy(
                src_ref=view(block, core),
                dst_ref=view(block, core),
                send_sem=ici_send.at[stage],
                recv_sem=recv.at[block],
                device_id=(dp, dest),
                device_id_type=MESH,
            )

        def start(block, dest):
            ici(block, dest).start()

        def wait(block):
            ici(block, lax.rem(me + 1, SEQ)).wait_recv()

        def arrived(block):
            if shared is not None:
                pltpu.make_async_remote_copy(
                    src_ref=view(block, core),
                    dst_ref=view(block, core),
                    send_sem=d2d_send.at[shared],
                    recv_sem=d2d_recv.at[shared],
                    device_id=(partner, me),
                    device_id_type=MESH,
                ).start()

        zfirst = ring_steps(z, x, NZ, NX, lambda p, q: q * NZ + p, start, wait, arrived)
        xfirst = ring_steps(x, z, NX, NZ, lambda p, q: p * NZ + q, start, wait, arrived)

        def run(low, high):
            @pl.when(core == 0)
            def _():
                for step in zfirst[low:high]:
                    step()

            @pl.when(core == 1)
            def _():
                for step in xfirst[low:high]:
                    step()

        return run, len(zfirst)

    def drain(whole, stage, shared):
        pltpu.make_async_copy(whole, whole, ici_send.at[stage]).wait()
        if shared is not None:
            pltpu.make_async_copy(whole, whole, d2d_send.at[shared]).wait()
            pltpu.make_async_copy(whole, whole, d2d_recv.at[shared]).wait()

    def half_rows(block, half):
        start = block * DEPTH + half * HALF
        return pl.ds(pl.multiple_of(start, HALF), HALF)

    w_run, w_steps = gather(lambda s, c: weights.at[half_rows(s, c), :], w_recv, 0, 0)
    o_run, o_steps = gather(lambda s, c: wots.at[half_rows(s, c), :], o_recv, 1, 1)
    kv_run, kv_steps = gather(
        lambda s, c: kv.at[pl.ds(pl.multiple_of(s * ROWS, ROWS), ROWS), :], kv_recv, 2, None
    )

    for copy in loads[:3]:
        copy.wait()
    w_run(0, 1)

    base = (me * TOK).astype(F32)
    listed = crow[...]
    first = jnp.sum(jnp.where(listed < base, 1.0, 0.0), axis=1, keepdims=True)
    last = jnp.sum(jnp.where(listed < base + TOK, 1.0, 0.0), axis=1, keepdims=True)
    shift = jnp.minimum(first, float(CHOSEN - MOST))

    def pick(i, carry):
        rows = pl.ds(pl.multiple_of(i * 32, 32), 32)
        lane = lax.broadcasted_iota(jnp.int32, (32, CHOSEN), 1).astype(F32)
        rank = lax.broadcasted_iota(jnp.int32, (32, 1), 0).astype(F32)
        hit = lane == rank + (shift + (i * 32).astype(F32))
        spot = jnp.sum(jnp.where(hit, crow[...], 0.0), axis=1, keepdims=True)
        gate = jnp.sum(jnp.where(hit, grow[...], 0.0), axis=1, keepdims=True)
        cpos[0, rows, :] = jnp.broadcast_to(spot, (32, 128))
        cpos[1, rows, :] = jnp.broadcast_to(gate, (32, 128))
        return carry

    lax.fori_loop(0, MOST // 32, pick, 0)
    spot = cpos[0, :, 0:1]
    gate = cpos[1, :, 0:1]
    eye = lax.broadcasted_iota(jnp.int32, (MOST, MOST), 0) == lax.broadcasted_iota(
        jnp.int32, (MOST, MOST), 1
    )
    meta[0:1, :] = jnp.sum(jnp.where(eye, spot - base, 0.0), axis=0, keepdims=True)
    meta[1:2, :] = jnp.sum(jnp.where(eye, gate, 0.0), axis=0, keepdims=True)
    place = lax.broadcasted_iota(jnp.int32, (MOST, TOK), 1).astype(F32)
    onehot[...] = jnp.where(place == spot - base, 1.0, 0.0).astype(BF16)

    token_load.wait()
    loads[3].wait()
    unit = jnp.where(
        lax.broadcasted_iota(jnp.int32, (DEPTH, DEPTH), 0)
        == lax.broadcasted_iota(jnp.int32, (DEPTH, DEPTH), 1),
        1.0,
        0.0,
    ).astype(BF16)
    wots[w_rows, :] = lax.dot_general(
        unit, wo_in[...], (((1,), (1,)), ((), ())), preferred_element_type=F32
    ).astype(BF16)

    def gather_rows(n, square):
        columns = pl.ds(pl.multiple_of(n * 256, 256), 256)
        part = jnp.dot(onehot[...], tok[:, columns], preferred_element_type=F32)
        normed[:, columns] = part.astype(BF16)
        return square + jnp.sum(part * part, axis=1, keepdims=True)

    square = lax.fori_loop(0, D // 256, gather_rows, jnp.zeros((MOST, 1), F32))
    scale = lax.rsqrt(square * (1.0 / D) + 1e-06)

    def normalize(n, carry):
        columns = pl.ds(pl.multiple_of(n * 256, 256), 256)
        normed[:, columns] = (normed[:, columns].astype(F32) * scale).astype(BF16)
        return carry

    lax.fori_loop(0, D // 256, normalize, 0)

    w_run(1, w_steps)
    drain(weights.at[pl.ds(0, HALF * (SEQ - 1)), :], 0, 0)

    def project_kv(n, carry):
        columns = pl.ds(pl.multiple_of(QW + n * 256, 256), 256)
        part = jnp.dot(normed[...], weights[:, columns], preferred_element_type=F32)
        query[:, pl.ds(pl.multiple_of(n * 256, 256), 256)] = part.astype(BF16)
        return carry

    lax.fori_loop(0, 2, project_kv, 0)

    order = lax.broadcasted_iota(jnp.int32, (MOST, MOST), 1)
    slot = lax.broadcasted_iota(jnp.int32, (MOST, MOST), 0)
    rank = order + shift.astype(jnp.int32)
    offset = rank - first.astype(jnp.int32)
    inside = jnp.where(offset >= 0, 1, 0) * jnp.where(rank < last.astype(jnp.int32), 1, 0)
    goes = (rank & (SEQ - 1)) * SLOTS + (offset >> 5)
    deal = jnp.where(goes == slot, inside, 0).astype(F32).astype(BF16)
    leaving = jnp.dot(deal, query[:, 0 : 2 * KW], preferred_element_type=F32)
    kv_slots[...] = leaving.reshape(SEQ, SLOTS, 2 * KW).astype(BF16)

    def slot_copy(j):
        dest = lax.rem(me + j, SEQ)
        return pltpu.make_async_remote_copy(
            src_ref=kv_slots.at[dest],
            dst_ref=kv_in.at[me],
            send_sem=a_send,
            recv_sem=a_recv,
            device_id=(dp, dest),
            device_id_type=MESH,
        )

    def send_slot(j, carry):
        slot_copy(j).start()
        return carry

    lax.fori_loop(1, SEQ, send_slot, 0)
    kv_in[me] = kv_slots[me]

    def project_q(n, carry):
        columns = pl.ds(pl.multiple_of(n * 256, 256), 256)
        part = jnp.dot(normed[...], weights[:, columns], preferred_element_type=F32)
        query[:, columns] = (part * HEAD_DIM ** (-0.5)).astype(BF16)
        return carry

    lax.fori_loop(0, QW // 256, project_q, 0)

    lane32 = lax.broadcasted_iota(jnp.int32, (ROWS, SEQ), 1)
    mine = jnp.sum(jnp.where(lane32 == me, c2[...], 0.0), axis=1, keepdims=True)
    source = jnp.floor(mine * (1.0 / TOK))

    def before(i, total):
        columns = pl.ds(pl.multiple_of(i * 1024, 1024), 1024)
        return total + jnp.sum(
            jnp.where(crow[:, columns] < source * TOK, 1.0, 0.0), axis=1, keepdims=True
        )

    starts = lax.fori_loop(0, CHOSEN // 1024, before, jnp.zeros((ROWS, 1), F32))
    my_rank = lax.broadcasted_iota(jnp.int32, (ROWS, 1), 0).astype(F32) * SEQ + me.astype(F32)
    found = source * SLOTS + jnp.floor((my_rank - starts) * (1.0 / SEQ))
    take = jnp.where(
        lax.broadcasted_iota(jnp.int32, (ROWS, MOST), 1).astype(F32) == found, 1.0, 0.0
    ).astype(BF16)

    def bias_block(i, carry):
        columns = pl.ds(pl.multiple_of(i * ROWS, ROWS), ROWS)
        bias[:, columns] = jnp.where(c2t[pl.ds(i, 1), :] <= spot, 0.0, FAR)
        return carry

    lax.fori_loop(0, SEQ, bias_block, 0)

    pltpu.make_async_copy(
        kv_in.at[pl.ds(0, SEQ - 1)], kv_in.at[pl.ds(0, SEQ - 1)], a_recv
    ).wait()
    came = kv_in[...].astype(F32).reshape(MOST, 2 * KW).astype(BF16)
    kv[pl.ds(pl.multiple_of(me * ROWS, ROWS), ROWS), :] = jnp.dot(
        take, came, preferred_element_type=F32
    ).astype(BF16)
    kv_run(0, kv_steps)
    o_run(0, 1)

    CHUNK = 1024
    done = 1
    for head in range(HEADS):
        e = head // GROUP
        q = query[:, head * HEAD_DIM : (head + 1) * HEAD_DIM]

        def one_chunk(i, state):
            top, total, acc = state
            rows = pl.ds(pl.multiple_of(i * CHUNK, CHUNK), CHUNK)
            keys = kv[rows, e * HEAD_DIM : (e + 1) * HEAD_DIM]
            values = kv[rows, KW + e * HEAD_DIM : KW + (e + 1) * HEAD_DIM]
            scores = lax.dot_general(
                q, keys, (((1,), (1,)), ((), ())), preferred_element_type=F32
            )
            scores = scores + bias[:, rows]
            fresh = jnp.maximum(top, jnp.max(scores, axis=1, keepdims=True))
            probs = jnp.exp(scores - fresh)
            shrink = jnp.exp(top - fresh)
            total = total * shrink + jnp.sum(probs, axis=1, keepdims=True)
            acc = acc * shrink + jnp.dot(
                probs.astype(BF16), values, preferred_element_type=F32
            )
            return fresh, total, acc

        state = (
            jnp.full((MOST, 1), FAR, F32),
            jnp.zeros((MOST, 1), F32),
            jnp.zeros((MOST, HEAD_DIM), F32),
        )
        top, total, acc = lax.fori_loop(0, CHOSEN // CHUNK, one_chunk, state)
        att[:, head * HEAD_DIM : (head + 1) * HEAD_DIM] = (acc / total).astype(BF16)
        until = 1 + (o_steps - 1) * (head + 1) // HEADS
        o_run(done, until)
        done = until

    drain(wots.at[pl.ds(0, HALF * (SEQ - 1)), :], 1, 1)
    pltpu.make_async_copy(
        kv.at[pl.ds(0, ROWS * (SEQ - 1)), :], kv.at[pl.ds(0, ROWS * (SEQ - 1)), :], ici_send.at[2]
    ).wait()
    pltpu.make_async_copy(
        kv_in.at[pl.ds(0, SEQ - 1)], kv_in.at[pl.ds(0, SEQ - 1)], a_send
    ).wait()

    def project_out(n, carry):
        columns = pl.ds(pl.multiple_of(n * 256, 256), 256)
        out[:, columns] = lax.dot_general(
            att[...], wots[columns, :], (((1,), (1,)), ((), ())), preferred_element_type=F32
        ).astype(BF16)
        return carry

    lax.fori_loop(0, D // 256, project_out, 0)


def mix_kernel(tile, tokens, block_out, meta, mixed):
    i = pl.program_id(0)
    place = lax.broadcasted_iota(jnp.int32, (tile, MOST), 0) + i * tile
    hit = place.astype(F32) == meta[0:1, :]
    gate = jnp.sum(jnp.where(hit, meta[1:2, :], 0.0), axis=1, keepdims=True)
    chosen_row = jnp.where(hit, 1.0, 0.0).astype(BF16)
    for n in range(D // 256):
        columns = slice(n * 256, (n + 1) * 256)
        rows = jnp.dot(chosen_row, block_out[:, columns], preferred_element_type=F32)
        mixed[:, columns] = (tokens[:, columns].astype(F32) + gate * rows).astype(BF16)


def per_device(tokens, chosen, gates, w_query, w_key, w_value, w_out):
    spots = chosen.astype(F32)
    c2 = spots.reshape(ROWS, SEQ)
    anywhere = pl.BlockSpec(memory_space=pl.ANY)
    inside = pl.BlockSpec(memory_space=pltpu.VMEM)
    dma = pltpu.SemaphoreType.DMA
    block_out, meta = pl.pallas_call(
        block_kernel,
        out_shape=(
            jax.ShapeDtypeStruct((MOST, D), BF16),
            jax.ShapeDtypeStruct((8, MOST), F32),
        ),
        in_specs=[anywhere] * 5 + [inside] * 4,
        out_specs=(inside, inside),
        scratch_shapes=[
            pltpu.VMEM((TOK, D), BF16),
            pltpu.VMEM((D, W), BF16),
            pltpu.VMEM((D, QW), BF16),
            pltpu.VMEM((QW, DEPTH), BF16),
            pltpu.VMEM((MOST, D), BF16),
            pltpu.VMEM((MOST, TOK), BF16),
            pltpu.VMEM((MOST, CHOSEN), F32),
            pltpu.VMEM((MOST, QW), BF16),
            pltpu.VMEM((MOST, QW), BF16),
            pltpu.VMEM((SEQ, SLOTS, 2 * KW), BF16),
            pltpu.VMEM((SEQ, SLOTS, 2 * KW), BF16),
            pltpu.VMEM((CHOSEN, 2 * KW), BF16),
            pltpu.VMEM((2, MOST, 128), F32),
            pltpu.SemaphoreType.REGULAR,
            dma((4,)),
            dma,
            dma((3,)),
            dma((SEQ,)),
            dma((SEQ,)),
            dma((SEQ,)),
            dma,
            dma,
            dma((2,)),
            dma((2,)),
        ],
        compiler_params=pltpu.CompilerParams(
            collective_id=0, has_side_effects=True, vmem_limit_bytes=56 * 1024 * 1024
        ),
        name="block",
    )(
        tokens, w_query, w_key, w_value, w_out,
        spots.reshape(1, CHOSEN), gates.reshape(1, CHOSEN), c2, c2.T,
    )
    tile = 256
    return pl.pallas_call(
        functools.partial(mix_kernel, tile),
        grid=(TOK // tile,),
        out_shape=jax.ShapeDtypeStruct((TOK, D), BF16),
        in_specs=[
            pl.BlockSpec((tile, D), lambda i: (i, 0)),
            pl.BlockSpec((MOST, D), lambda i: (0, 0)),
            pl.BlockSpec((8, MOST), lambda i: (0, 0)),
        ],
        out_specs=pl.BlockSpec((tile, D), lambda i: (i, 0)),
        name="mix",
    )(tokens, block_out, meta)


def solution(mesh):
    return jax.shard_map(
        per_device,
        mesh=mesh,
        in_specs=(
            P(("dp", "seq"), None),
            P("dp"),
            P("dp"),
            P("seq", None),
            P("seq", None),
            P("seq", None),
            P(None, "seq"),
        ),
        out_specs=P(("dp", "seq"), None),
        check_vma=False,
    )
```

```python
import functools

import jax
import jax.numpy as jnp
from jax import lax
from jax.experimental import pallas as pl
from jax.experimental.pallas import tpu as pltpu
from jax.sharding import PartitionSpec as P

HEADS = 8
KV_HEADS = 2
GROUP = HEADS // KV_HEADS
HEAD_DIM = 128
D = 2048
QW = HEADS * HEAD_DIM
KW = KV_HEADS * HEAD_DIM
SEQ = 32
NX = 4
NZ = 8
TOK = 1024
CHOSEN = 4096
ROWS = 128
MOST = 256
SLOTS = 8
DEPTH = D // SEQ
HALF = DEPTH // 2
PARTS = 8
PIECE = DEPTH // PARTS
CHUNK = 1024
PER = CHUNK // ROWS
LAG = 4
MESH = pl.DeviceIdType.MESH
F32 = jnp.float32
BF16 = jnp.bfloat16
FAR = -1e30


def ring_steps(na, nb, send, wait, arrived):
    def reach(order, n):
        return (n // 2, n // 2 - 1) if order % 2 == 0 else (n // 2 - 1, n // 2)

    def first():
        for to in ((1, 0), (-1, 0), (0, 1), (0, -1)):
            send((0, 0), to)

    def along_a(k, side):
        block = (-side * k, 0)
        wait(block)
        if k < reach(0, na)[0 if side == 1 else 1]:
            send(block, (side, 0))
        send(block, (0, 1))
        send(block, (0, -1))
        arrived(block)

    def along_b(order, j, m, side):
        block = (j, -side * m)
        wait(block)
        if m < reach(order, nb)[0 if side == 1 else 1]:
            send(block, (0, side))
        arrived(block)

    steps, blocks, columns = [first], [(0, 0)], [0]
    for k in range(1, na // 2 + 1):
        for side in (1, -1):
            if k <= reach(0, na)[0 if side == 1 else 1]:
                steps.append(functools.partial(along_a, k, side))
                columns.append(-side * k)
                blocks.append((-side * k, 0))
    for m in range(1, nb // 2 + 1):
        for order, j in enumerate(columns):
            for side in (1, -1):
                if m <= reach(order, nb)[0 if side == 1 else 1]:
                    steps.append(functools.partial(along_b, order, j, m, side))
                    blocks.append((j, -side * m))
    return steps, [(p % na, q % nb) for p, q in blocks]


def block_kernel(
    tokens, wq, wk, wv, wo, crow, grow, c2, c2t,
    out, meta,
    tok, kvw, wqo, normed, onehot, deal, take, bias, query, att, kv_own, kv_slots, kv_in, kv,
    cpos, wide, top_ref, total_ref, acc_ref,
    load_sem, tok_sem, w_send, w_recv, o_send, o_recv, d_send, d_recv, a_send, a_recv,
    kv_send, kv_recv, q_send, q_recv, y_send, y_recv, p_send, p_recv,
):
    dp = lax.axis_index("dp")
    me = lax.axis_index("seq")
    core = lax.rem(dp, 2)
    y = dp // 2
    partner = dp + 1 - 2 * core
    x, z = me // NZ, lax.rem(me, NZ)

    def along_y(k):
        return lax.rem(y + k + 4, 4) * 2 + core

    def zf(block):
        return lax.rem(x + block[1] + NX, NX) * NZ + lax.rem(z + block[0] + NZ, NZ)

    def xf(block):
        return lax.rem(x + block[0] + NX, NX) * NZ + lax.rem(z + block[1] + NZ, NZ)

    def remote(src, dst, send_sem, recv_sem, to_dp, to_seq):
        return pltpu.make_async_remote_copy(
            src_ref=src,
            dst_ref=dst,
            send_sem=send_sem,
            recv_sem=recv_sem,
            device_id=(to_dp, to_seq),
            device_id_type=MESH,
        )

    def kv_unit(s, half):
        start = s * DEPTH + half * HALF
        return pl.ds(pl.multiple_of(start, HALF), HALF)

    own = kv_unit(me, core)
    loads = [
        pltpu.make_async_copy(wk.at[pl.ds(core * HALF, HALF), :], kvw.at[own, 0:KW], load_sem.at[0]),
        pltpu.make_async_copy(wv.at[pl.ds(core * HALF, HALF), :], kvw.at[own, KW : 2 * KW], load_sem.at[1]),
        pltpu.make_async_copy(wq.at[dp], wqo.at[0, me, dp], load_sem.at[2]),
        pltpu.make_async_copy(wo.at[dp], wqo.at[1, me, dp], load_sem.at[3]),
    ]
    for copy in loads:
        copy.start()
    token_load = pltpu.make_async_copy(tokens, tok, tok_sem)
    token_load.start()

    barrier = pltpu.get_barrier_semaphore()

    def greet(j, carry):
        pl.semaphore_signal(
            barrier, inc=1, device_id=(dp, lax.rem(me + j, SEQ)), device_id_type=MESH
        )
        return carry

    lax.fori_loop(1, SEQ, greet, 0)
    for other in (partner, along_y(1), along_y(-1)):
        pl.semaphore_signal(barrier, inc=1, device_id=(other, me), device_id_type=MESH)

    base = (me * TOK).astype(F32)
    listed = crow[...]
    first = jnp.sum(jnp.where(listed < base, 1.0, 0.0), axis=1, keepdims=True)
    last = jnp.sum(jnp.where(listed < base + TOK, 1.0, 0.0), axis=1, keepdims=True)
    shift = jnp.minimum(first, float(CHOSEN - MOST))

    def pick(i, carry):
        rows = pl.ds(pl.multiple_of(i * 32, 32), 32)
        lane = lax.broadcasted_iota(jnp.int32, (32, CHOSEN), 1).astype(F32)
        rank = lax.broadcasted_iota(jnp.int32, (32, 1), 0).astype(F32)
        hit = lane == rank + (shift + (i * 32).astype(F32))
        spot = jnp.sum(jnp.where(hit, crow[...], 0.0), axis=1, keepdims=True)
        gate = jnp.sum(jnp.where(hit, grow[...], 0.0), axis=1, keepdims=True)
        cpos[0, rows, :] = jnp.broadcast_to(spot, (32, 128))
        cpos[1, rows, :] = jnp.broadcast_to(gate, (32, 128))
        return carry

    lax.fori_loop(0, MOST // 32, pick, 0)
    place = lax.broadcasted_iota(jnp.int32, (MOST, TOK), 1).astype(F32)
    onehot[...] = jnp.where(place == cpos[0, :, 0:1] - base, 1.0, 0.0).astype(BF16)

    for copy in loads:
        copy.wait()
    pl.semaphore_wait(barrier, SEQ + 2)

    def q_copy(s, k, slot, to):
        piece = wqo.at[0, s, along_y(k)]
        return remote(piece, piece, q_send, q_recv.at[slot, s], along_y(to), me)

    def to_y(s):
        q_copy(s, 0, 0, 1).start()
        q_copy(s, 0, 1, -1).start()

    def from_y(i):
        s = block_at(i)
        q_copy(s, -1, 0, 1).wait_recv()
        if i % 2 == 0:
            q_copy(s, -1, 2, 1).start()
        q_copy(s, 1, 1, -1).wait_recv()
        if i % 2 == 1:
            q_copy(s, 1, 2, -1).start()

    def first_gather(at):
        def send(block, to):
            s, dest = at(block), at(to)
            half = kvw.at[kv_unit(s, core), :]
            remote(half, half, w_send, w_recv.at[s], dp, dest).start()
            part = wqo.at[:, s, dp]
            remote(part, part, o_send, o_recv.at[s], dp, dest).start()

        def wait(block):
            s, other = at(block), lax.rem(me + 1, SEQ)
            half = kvw.at[kv_unit(s, core), :]
            remote(half, half, w_send, w_recv.at[s], dp, other).wait_recv()
            part = wqo.at[:, s, dp]
            remote(part, part, o_send, o_recv.at[s], dp, other).wait_recv()

        def arrived(block):
            s = at(block)
            half = kvw.at[kv_unit(s, core), :]
            remote(half, half, d_send, d_recv, partner, me).start()
            to_y(s)

        return send, wait, arrived

    def by_core(z_steps, x_steps):
        @pl.when(core == 0)
        def _():
            for step in z_steps:
                step()

        @pl.when(core == 1)
        def _():
            for step in x_steps:
                step()

    z_steps, z_blocks = ring_steps(NZ, NX, *first_gather(zf))
    x_steps, x_blocks = ring_steps(NX, NZ, *first_gather(xf))

    def block_at(i):
        return jnp.where(core == 0, zf(z_blocks[i]), xf(x_blocks[i]))

    def gather_rows(n):
        columns = slice(n * 256, (n + 1) * 256)
        part = jnp.dot(onehot[...], tok[:, columns], preferred_element_type=F32)
        normed[:, columns] = part.astype(BF16)
        square = jnp.broadcast_to(jnp.sum(part * part, axis=1, keepdims=True), (MOST, 128))
        wide[...] = square if n == 0 else wide[...] + square

    def normalize(n):
        columns = slice(n * 512, (n + 1) * 512)
        scale = lax.rsqrt(wide[:, 0:1] * (1.0 / D) + 1e-06)
        normed[:, columns] = (normed[:, columns].astype(F32) * scale).astype(BF16)

    def place_rows():
        order = lax.broadcasted_iota(jnp.int32, (MOST, MOST), 1)
        slot = lax.broadcasted_iota(jnp.int32, (MOST, MOST), 0)
        rank = order + shift.astype(jnp.int32)
        offset = rank - first.astype(jnp.int32)
        inside = jnp.where(offset >= 0, 1, 0) * jnp.where(rank < last.astype(jnp.int32), 1, 0)
        goes = (rank & (SEQ - 1)) * SLOTS + (offset >> 5)
        deal[...] = jnp.where(goes == slot, inside, 0).astype(F32).astype(BF16)
        gate = cpos[1, :, 0:1]
        eye = order == slot
        meta[0:1, :] = jnp.sum(jnp.where(eye, cpos[0, :, 0:1] - base, 0.0), axis=0, keepdims=True)
        meta[1:2, :] = jnp.sum(jnp.where(eye, gate, 0.0), axis=0, keepdims=True)

    def find_slots():
        lane32 = lax.broadcasted_iota(jnp.int32, (ROWS, SEQ), 1)
        mine = jnp.sum(jnp.where(lane32 == me, c2[...], 0.0), axis=1, keepdims=True)
        source = jnp.floor(mine * (1.0 / TOK))

        def before(i, total):
            columns = pl.ds(pl.multiple_of(i * 512, 512), 512)
            return total + jnp.sum(
                jnp.where(crow[:, columns] < source * TOK, 1.0, 0.0), axis=1, keepdims=True
            )

        starts = lax.fori_loop(0, CHOSEN // 512, before, jnp.zeros((ROWS, 1), F32))
        my_rank = lax.broadcasted_iota(jnp.int32, (ROWS, 1), 0).astype(F32) * SEQ + me.astype(F32)
        found = source * SLOTS + jnp.floor((my_rank - starts) * (1.0 / SEQ))
        take[...] = jnp.where(
            lax.broadcasted_iota(jnp.int32, (ROWS, MOST), 1).astype(F32) == found, 1.0, 0.0
        ).astype(BF16)

    def bias_blocks(low, high):
        for slot in range(low, high):
            s = block_at(slot)
            bias[:, slot * ROWS : (slot + 1) * ROWS] = jnp.where(
                c2t[pl.ds(s, 1), :] <= cpos[0, :, 0:1], 0.0, FAR
            )

    work = [functools.partial(gather_rows, n) for n in range(D // 256)]
    work += [functools.partial(normalize, n) for n in range(D // 512)]
    work += [place_rows, find_slots]
    work += [functools.partial(bias_blocks, n, n + 4) for n in range(0, SEQ, 4)]

    by_core(z_steps[0:1], x_steps[0:1])
    half = kvw.at[own, :]
    remote(half, half, d_send, d_recv, partner, me).start()
    to_y(me)
    token_load.wait()
    for i in range(1, SEQ):
        if i <= len(work):
            work[i - 1]()
        by_core(z_steps[i : i + 1], x_steps[i : i + 1])
        if i >= LAG:
            from_y(i - LAG)
    for rest in work[SEQ - 1 :]:
        rest()

    def part(a, k, low=0, high=SEQ):
        return wqo.at[a, pl.ds(low, high - low), along_y(k)]

    def along(a, k, slot, to, low=0, high=SEQ):
        return remote(
            part(a, k, low, high), part(a, k, low, high), y_send, y_recv.at[a, slot], along_y(to), me
        )

    def across(a, k):
        remote(part(a, k), part(a, k), p_send, p_recv.at[a], partner, me).start()

    def y_first(a):
        along(a, 0, 0, 1).start()
        along(a, 0, 1, -1).start()
        across(a, 0)

    def y_second(a):
        along(a, -1, 0, 1).wait_recv()
        along(a, -1, 2, 1, 0, SEQ // 2).start()
        across(a, -1)
        along(a, 1, 1, -1).wait_recv()
        along(a, 1, 3, -1, SEQ // 2, SEQ).start()
        across(a, 1)

    def y_third(a):
        along(a, 2, 2, 1, 0, SEQ // 2).wait_recv()
        along(a, 2, 3, -1, SEQ // 2, SEQ).wait_recv()
        across(a, 2)

    def y_last(a):
        whole = wqo.at[a, :, pl.ds(0, 4)]
        pltpu.make_async_copy(whole, whole, p_recv.at[a]).wait()

    whole = kvw.at[pl.ds(0, HALF * SEQ), :]
    pltpu.make_async_copy(whole, whole, d_recv).wait()

    for n in range(2):
        columns = slice(n * 256, (n + 1) * 256)
        kv_own[:, columns] = jnp.dot(
            normed[...], kvw[:, columns], preferred_element_type=F32
        ).astype(BF16)
    leaving = jnp.dot(deal[...], kv_own[...], preferred_element_type=F32)
    kv_slots[...] = leaving.reshape(SEQ, SLOTS, 2 * KW).astype(BF16)

    def send_slot(j, carry):
        dest = lax.rem(me + j, SEQ)
        remote(kv_slots.at[dest], kv_in.at[me], a_send, a_recv, dp, dest).start()
        return carry

    lax.fori_loop(1, SEQ, send_slot, 0)
    kv_in[me] = kv_slots[me]

    for i in range(SEQ - LAG, SEQ):
        from_y(i)

    def last_of_y(s, carry):
        q_copy(s, 2, 2, 1).wait_recv()
        return carry

    lax.fori_loop(0, SEQ, last_of_y, 0)
    for k in range(4):
        across(0, k)
    y_first(1)

    whole = kv_in.at[pl.ds(0, SEQ - 1)]
    pltpu.make_async_copy(whole, whole, a_recv).wait()
    came = kv_in[...].astype(F32).reshape(MOST, 2 * KW).astype(BF16)
    kv[0:ROWS, :] = jnp.dot(take[...], came, preferred_element_type=F32).astype(BF16)

    def second_gather(at, na, nb, blocks):
        def slot(block, seen_from=(0, 0)):
            return blocks.index(((block[0] - seen_from[0]) % na, (block[1] - seen_from[1]) % nb))

        def rows(n):
            return kv.at[pl.ds(n * ROWS, ROWS), :]

        def send(block, to):
            lands = slot(block, to)
            remote(rows(slot(block)), rows(lands), kv_send, kv_recv.at[lands], dp, at(to)).start()

        def wait(block):
            n = slot(block)
            remote(rows(n), rows(n), kv_send, kv_recv.at[n], dp, lax.rem(me + 1, SEQ)).wait_recv()

        return send, wait, lambda block: None

    zk_steps, _ = ring_steps(NZ, NX, *second_gather(zf, NZ, NX, z_blocks))
    xk_steps, _ = ring_steps(NX, NZ, *second_gather(xf, NX, NZ, x_blocks))

    def attend(g, h):
        columns = pl.ds(pl.multiple_of(h * HEAD_DIM, HEAD_DIM), HEAD_DIM)
        e = h // GROUP
        k_columns = pl.ds(pl.multiple_of(e * HEAD_DIM, HEAD_DIM), HEAD_DIM)
        v_columns = pl.ds(pl.multiple_of(KW + e * HEAD_DIM, HEAD_DIM), HEAD_DIM)
        rows = slice(g * CHUNK, (g + 1) * CHUNK)
        scores = lax.dot_general(
            query[:, columns], kv[rows, k_columns], (((1,), (1,)), ((), ())),
            preferred_element_type=F32,
        )
        scores = scores + bias[:, rows]
        fresh = jnp.max(scores, axis=1, keepdims=True)
        if g > 0:
            before = top_ref[h][:, 0:1]
            fresh = jnp.maximum(before, fresh)
        probs = jnp.exp(scores - fresh)
        total = jnp.sum(probs, axis=1, keepdims=True)
        acc = jnp.dot(probs.astype(BF16), kv[rows, v_columns], preferred_element_type=F32)
        if g > 0:
            shrink = jnp.exp(before - fresh)
            total = total_ref[h][:, 0:1] * shrink + total
            acc = acc_ref[h] * shrink + acc
        if g < CHOSEN // CHUNK - 1:
            top_ref[h] = jnp.broadcast_to(fresh, (MOST, 128))
            total_ref[h] = jnp.broadcast_to(total, (MOST, 128))
            acc_ref[h] = acc
        else:
            att[:, columns] = (acc / total).astype(BF16)

    def project_q():
        def tile(n, carry):
            columns = pl.ds(pl.multiple_of(n * 256, 256), 256)
            weights = wqo[0, :, :, :, columns].reshape(D, 256)
            piece = jnp.dot(normed[...], weights, preferred_element_type=F32)
            query[:, columns] = (piece * HEAD_DIM ** (-0.5)).astype(BF16)
            return carry

        lax.fori_loop(0, QW // 256, tile, 0)

    for g in range(CHOSEN // CHUNK + 1):
        if g == 0:
            by_core(zk_steps[0:1], xk_steps[0:1])
            y_last(0)
            project_q()
        if g == 2:
            y_second(1)

        def together(i, carry):
            if g < CHOSEN // CHUNK:
                for j in range(1 if g == 0 else 0, PER):

                    @pl.when(i == j)
                    def _():
                        n = g * PER + j
                        by_core(zk_steps[n : n + 1], xk_steps[n : n + 1])

            if g > 0:
                attend(g - 1, i)
            return carry

        lax.fori_loop(0, PER, together, 0)
        if g == 3:
            y_third(1)

    y_last(1)

    def project_out(n, carry):
        columns = pl.ds(pl.multiple_of(n * 256, 256), 256)
        weights = wqo[1, pl.ds(n * 4, 4)].reshape(256, QW)
        out[:, columns] = lax.dot_general(
            att[...], weights, (((1,), (1,)), ((), ())), preferred_element_type=F32
        ).astype(BF16)
        return carry

    lax.fori_loop(0, D // 256, project_out, 0)

    for whole, sem in (
        (kvw.at[pl.ds(0, HALF * (SEQ - 1)), :], w_send),
        (kvw.at[pl.ds(0, HALF * SEQ), :], d_send),
        (wqo.at[:, pl.ds(0, SEQ - 1), 0], o_send),
        (kv_in.at[pl.ds(0, SEQ - 1)], a_send),
        (kv.at[pl.ds(0, ROWS * (SEQ - 1)), :], kv_send),
        (wqo.at[0, :, pl.ds(0, 3)], q_send),
        (wqo.at[1, :, pl.ds(0, 3)], y_send),
        (wqo.at[:, :, pl.ds(0, 4)], p_send),
    ):
        pltpu.make_async_copy(whole, whole, sem).wait()


def mix_kernel(tile, tokens, block_out, meta, mixed):
    i = pl.program_id(0)
    place = lax.broadcasted_iota(jnp.int32, (tile, MOST), 0) + i * tile
    hit = place.astype(F32) == meta[0:1, :]
    gate = jnp.sum(jnp.where(hit, meta[1:2, :], 0.0), axis=1, keepdims=True)
    chosen_row = jnp.where(hit, 1.0, 0.0).astype(BF16)
    for n in range(D // 256):
        columns = slice(n * 256, (n + 1) * 256)
        rows = jnp.dot(chosen_row, block_out[:, columns], preferred_element_type=F32)
        mixed[:, columns] = (tokens[:, columns].astype(F32) + gate * rows).astype(BF16)


def per_device(tokens, chosen, gates, w_query, w_key, w_value, w_out):
    spots = chosen.astype(F32)
    c2 = spots.reshape(ROWS, SEQ)
    anywhere = pl.BlockSpec(memory_space=pl.ANY)
    inside = pl.BlockSpec(memory_space=pltpu.VMEM)
    dma = pltpu.SemaphoreType.DMA
    vmem = pltpu.VMEM
    block_out, meta = pl.pallas_call(
        block_kernel,
        out_shape=(
            jax.ShapeDtypeStruct((MOST, D), BF16),
            jax.ShapeDtypeStruct((8, MOST), F32),
        ),
        in_specs=[anywhere] * 5 + [inside] * 4,
        out_specs=(inside, inside),
        scratch_shapes=[
            vmem((TOK, D), BF16),
            vmem((D, 2 * KW), BF16),
            vmem((2, SEQ, PARTS, PIECE, QW), BF16),
            vmem((MOST, D), BF16),
            vmem((MOST, TOK), BF16),
            vmem((MOST, MOST), BF16),
            vmem((ROWS, MOST), BF16),
            vmem((MOST, CHOSEN), F32),
            vmem((MOST, QW), BF16),
            vmem((MOST, QW), BF16),
            vmem((MOST, 2 * KW), BF16),
            vmem((SEQ, SLOTS, 2 * KW), BF16),
            vmem((SEQ, SLOTS, 2 * KW), BF16),
            vmem((CHOSEN, 2 * KW), BF16),
            vmem((2, MOST, 128), F32),
            vmem((MOST, 128), F32),
            vmem((HEADS, MOST, 128), F32),
            vmem((HEADS, MOST, 128), F32),
            vmem((HEADS, MOST, 128), F32),
            dma((4,)),
            dma,
            dma,
            dma((SEQ,)),
            dma,
            dma((SEQ,)),
            dma,
            dma,
            dma,
            dma,
            dma,
            dma((SEQ,)),
            dma,
            dma((3, SEQ)),
            dma,
            dma((2, 4)),
            dma,
            dma((2,)),
        ],
        compiler_params=pltpu.CompilerParams(
            collective_id=0, has_side_effects=True, vmem_limit_bytes=56 * 1024 * 1024
        ),
        name="block",
    )(
        tokens,
        w_query.reshape(PARTS, PIECE, QW),
        w_key,
        w_value,
        w_out.T.reshape(PARTS, PIECE, QW),
        spots.reshape(1, CHOSEN),
        gates.reshape(1, CHOSEN),
        c2,
        c2.T,
    )
    tile = 256
    return pl.pallas_call(
        functools.partial(mix_kernel, tile),
        grid=(TOK // tile,),
        out_shape=jax.ShapeDtypeStruct((TOK, D), BF16),
        in_specs=[
            pl.BlockSpec((tile, D), lambda i: (i, 0)),
            pl.BlockSpec((MOST, D), lambda i: (0, 0)),
            pl.BlockSpec((8, MOST), lambda i: (0, 0)),
        ],
        out_specs=pl.BlockSpec((tile, D), lambda i: (i, 0)),
        name="mix",
    )(tokens, block_out, meta)


def solution(mesh):
    return jax.shard_map(
        per_device,
        mesh=mesh,
        in_specs=(
            P(("dp", "seq"), None),
            P("dp"),
            P("dp"),
            P("seq", None),
            P("seq", None),
            P("seq", None),
            P(None, "seq"),
        ),
        out_specs=P(("dp", "seq"), None),
        check_vma=False,
    )
```

```python
import functools

import jax
import jax.numpy as jnp
from jax import lax
from jax.experimental import pallas as pl
from jax.experimental.pallas import tpu as pltpu
from jax.sharding import PartitionSpec as P

HEADS = 8
KV_HEADS = 2
GROUP = HEADS // KV_HEADS
HEAD_DIM = 128
D = 2048
QW = HEADS * HEAD_DIM
KW = KV_HEADS * HEAD_DIM
SEQ = 32
NX = 4
NZ = 8
TOK = 1024
CHOSEN = 4096
ROWS = 128
MOST = 256
SLOTS = 8
DEPTH = D // SEQ
HALF = DEPTH // 2
PARTS = 8
PIECE = DEPTH // PARTS
CHUNK = 1024
PER = CHUNK // ROWS
SIDE = ROWS // 2
EARLY = 5
PAIR = 2
TILE = 256
TILES = TOK // TILE
MESH = pl.DeviceIdType.MESH
F32 = jnp.float32
BF16 = jnp.bfloat16
FAR = -1e30


def ring_groups(na, nb):
    columns = [0]
    for k in range(1, na // 2 + 1):
        columns += [-k, k] if k < na // 2 else [-k]
    groups = [[(0, 0)]] + [[(j, 0)] for j in columns[1:]]
    for m in range(1, nb // 2):
        groups += [[(j, -m), (j, m)] for j in columns]
    return groups + [[(j, far_side(n) * -(nb // 2)) for n, j in enumerate(columns)]], columns


def far_side(order):
    return 1 if order % 2 == 0 else -1


def ring_steps(na, nb, direct, send, wait):
    groups, columns = ring_groups(na, nb)

    def first():
        along = [(-p, 0) for p in columns[1:]] if direct else [(1, 0), (-1, 0)]
        for to in along + [(0, 1), (0, -1)]:
            send((0, 0), to)

    def step(index):
        wait(index)
        for j, m in groups[index]:
            if m == 0:
                side = -1 if j > 0 else 1
                if not direct and abs(j) < (na // 2 if side == 1 else na // 2 - 1):
                    send((j, m), (side, 0))
                send((j, m), (0, 1))
                send((j, m), (0, -1))
            else:
                side = -1 if m > 0 else 1
                reach = nb // 2 if side == far_side(columns.index(j)) else nb // 2 - 1
                if abs(m) < reach:
                    send((j, m), (0, side))

    return [first] + [functools.partial(step, n) for n in range(1, len(groups))]


def places(na, nb):
    flat = {}
    for index, group in enumerate(ring_groups(na, nb)[0]):
        for j, m in group:
            flat[j % na, m % nb] = (len(flat), index)
    return flat


def block_kernel(
    tokens, wq, wk, wv, wo, crow, grow, listed_in,
    out, meta_out,
    out_tile, meta, tok, kvw, wqo, normed, onehot, deal, take, bias, query, att, kv_own, kv_slots, kv_in, kv,
    cpos, spots_f, c2t, wide, top_ref, total_ref, acc_ref,
    load_sem, tok_sem, out_sem, w_send, w_recv, o_send, o_recv, d_send, d_recv, a_send, a_recv,
    kv_send, kv_recv, q_send, q_recv, y_send, y_recv, p_send, p_recv,
):
    dp = lax.axis_index("dp")
    me = lax.axis_index("seq")
    core = lax.rem(dp, 2)
    y = dp // 2
    partner = dp + 1 - 2 * core
    x, z = me // NZ, lax.rem(me, NZ)

    def along_y(k):
        return lax.rem(y + k + 4, 4) * 2 + core

    def zf(block):
        return lax.rem(x + block[1] + NX, NX) * NZ + lax.rem(z + block[0] + NZ, NZ)

    def xf(block):
        return lax.rem(x + block[0] + NX, NX) * NZ + lax.rem(z + block[1] + NZ, NZ)

    def remote(src, dst, send_sem, recv_sem, to_dp, to_seq):
        return pltpu.make_async_remote_copy(
            src_ref=src,
            dst_ref=dst,
            send_sem=send_sem,
            recv_sem=recv_sem,
            device_id=(to_dp, to_seq),
            device_id_type=MESH,
        )

    def kv_unit(s, half):
        start = s * DEPTH + half * HALF
        return pl.ds(pl.multiple_of(start, HALF), HALF)

    own = kv_unit(me, core)
    loads = [
        pltpu.make_async_copy(wk.at[pl.ds(core * HALF, HALF), :], kvw.at[own, 0:KW], load_sem.at[0]),
        pltpu.make_async_copy(wv.at[pl.ds(core * HALF, HALF), :], kvw.at[own, KW : 2 * KW], load_sem.at[1]),
        pltpu.make_async_copy(wq.at[dp], wqo.at[0, me, dp], load_sem.at[2]),
        pltpu.make_async_copy(wo.at[dp], wqo.at[1, me, dp], load_sem.at[3]),
    ]
    for copy in loads:
        copy.start()
    token_load = pltpu.make_async_copy(tokens, tok, tok_sem)
    token_load.start()

    barrier = pltpu.get_barrier_semaphore()

    def greet(j, carry):
        pl.semaphore_signal(
            barrier, inc=1, device_id=(dp, lax.rem(me + j, SEQ)), device_id_type=MESH
        )
        return carry

    lax.fori_loop(1, SEQ, greet, 0)
    for other in (partner, along_y(1), along_y(-1)):
        pl.semaphore_signal(barrier, inc=1, device_id=(other, me), device_id_type=MESH)

    base = (me * TOK).astype(F32)
    listed = crow[...].astype(F32)
    spots_f[...] = listed
    first = jnp.sum(jnp.where(listed < base, 1.0, 0.0), axis=1, keepdims=True)
    last = jnp.sum(jnp.where(listed < base + TOK, 1.0, 0.0), axis=1, keepdims=True)
    shift = jnp.minimum(first, float(CHOSEN - MOST))

    def pick(i, carry):
        rows = pl.ds(pl.multiple_of(i * 32, 32), 32)
        lane = lax.broadcasted_iota(jnp.int32, (32, CHOSEN), 1).astype(F32)
        rank = lax.broadcasted_iota(jnp.int32, (32, 1), 0).astype(F32)
        hit = lane == rank + (shift + (i * 32).astype(F32))
        spot = jnp.sum(jnp.where(hit, spots_f[...], 0.0), axis=1, keepdims=True)
        gate = jnp.sum(jnp.where(hit, grow[...], 0.0), axis=1, keepdims=True)
        cpos[0, rows, :] = jnp.broadcast_to(spot, (32, 128))
        cpos[1, rows, :] = jnp.broadcast_to(gate, (32, 128))
        return carry

    lax.fori_loop(0, MOST // 32, pick, 0)
    place = lax.broadcasted_iota(jnp.int32, (MOST, TOK), 1).astype(F32)
    onehot[...] = jnp.where(place == cpos[0, :, 0:1] - base, 1.0, 0.0).astype(BF16)

    for copy in loads:
        copy.wait()
    pl.semaphore_wait(barrier, SEQ + 2)

    z_places, x_places = places(NZ, NX), places(NX, NZ)
    z_blocks, x_blocks = list(z_places), list(x_places)

    def block_at(i):
        return zf(z_blocks[i])

    def q_copy(s, k, sem, to):
        piece = wqo.at[0, s, along_y(k)]
        return remote(piece, piece, q_send, q_recv.at[sem], along_y(to), me)

    def to_y(n):
        s = block_at(n)
        q_copy(s, 0, n // 2, 1).start()
        q_copy(s, 0, n // 2, -1).start()
        q_across(s, 0)

    def q_across(s, k):
        piece = wqo.at[0, s, along_y(k)]
        remote(piece, piece, p_send, p_recv.at[0], partner, me).start()

    def from_y(i):
        both = wqo.at[0, pl.ds(0, 4), 0]
        pltpu.make_async_copy(both, both, q_recv.at[i]).wait()
        low, high = block_at(2 * i), block_at(2 * i + 1)
        q_copy(low, -1, SEQ // 2, 1).start()
        q_copy(high, 1, SEQ // 2, -1).start()
        for s in (low, high):
            q_across(s, -1)
            q_across(s, 1)

    def first_gather(view, many, send_sem, recv_sem, arrived):
        groups = ring_groups(NZ, NX)[0]

        def send(block, to):
            group = z_places[(block[0] - to[0]) % NZ, (block[1] - to[1]) % NX][1]
            s = zf(block)
            remote(view(s), view(s), send_sem, recv_sem.at[group], dp, zf(to)).start()

        def wait(index):
            some = many(len(groups[index]))
            pltpu.make_async_copy(some, some, recv_sem.at[index]).wait()

        def then(index, step):
            step()
            for block in groups[index]:
                arrived(z_places[block[0] % NZ, block[1] % NX][0])

        steps = ring_steps(NZ, NX, True, send, wait)
        return [functools.partial(then, index, step) for index, step in enumerate(steps)]

    def kv_half(s):
        return kvw.at[kv_unit(s, core), :]

    def to_partner(n):
        half = kv_half(block_at(n))
        remote(half, half, d_send, d_recv, partner, me).start()

    w_steps = first_gather(
        kv_half, lambda n: kvw.at[pl.ds(0, n * HALF), :], w_send, w_recv, to_partner
    )
    o_steps = first_gather(
        lambda s: wqo.at[:, s, dp], lambda n: wqo.at[:, pl.ds(0, n), 0], o_send, o_recv, to_y
    )

    def gather_rows(n):
        columns = slice(n * 256, (n + 1) * 256)
        part = jnp.dot(onehot[...], tok[:, columns], preferred_element_type=F32)
        normed[:, columns] = part.astype(BF16)
        square = jnp.broadcast_to(jnp.sum(part * part, axis=1, keepdims=True), (MOST, 128))
        wide[...] = square if n == 0 else wide[...] + square

    def normalize(n):
        columns = slice(n * 512, (n + 1) * 512)
        scale = lax.rsqrt(wide[:, 0:1] * (1.0 / D) + 1e-06)
        normed[:, columns] = (normed[:, columns].astype(F32) * scale).astype(BF16)

    def place_rows():
        order = lax.broadcasted_iota(jnp.int32, (MOST, MOST), 1)
        slot = lax.broadcasted_iota(jnp.int32, (MOST, MOST), 0)
        rank = order + shift.astype(jnp.int32)
        offset = rank - first.astype(jnp.int32)
        inside = jnp.where(offset >= 0, 1, 0) * jnp.where(rank < last.astype(jnp.int32), 1, 0)
        goes = (rank & (SEQ - 1)) * SLOTS + (offset >> 5)
        deal[...] = jnp.where(goes == slot, inside, 0).astype(F32).astype(BF16)
        gate = cpos[1, :, 0:1]
        eye = order == slot
        meta[0:1, :] = jnp.sum(jnp.where(eye, cpos[0, :, 0:1] - base, 0.0), axis=0, keepdims=True)
        meta[1:2, :] = jnp.sum(jnp.where(eye, gate, 0.0), axis=0, keepdims=True)

    def dealt_order():
        rows = listed_in[...].astype(F32)
        r = lax.broadcasted_iota(jnp.int32, (SEQ, ROWS), 0)
        k = lax.broadcasted_iota(jnp.int32, (SEQ, ROWS), 1)
        for q in range(ROWS // SEQ):
            take_k = jnp.where(k == r * (ROWS // SEQ) + q, 1.0, 0.0)
            part = lax.dot_general(
                rows[:, q * SEQ : (q + 1) * SEQ], take_k, (((0,), (0,)), ((), ())),
                precision=lax.Precision.HIGHEST, preferred_element_type=F32,
            )
            c2t[...] = part if q == 0 else c2t[...] + part

    def find_slots():
        lane32 = lax.broadcasted_iota(jnp.int32, (ROWS, SEQ), 1)
        mine = jnp.sum(jnp.where(lane32 == me, c2t[...].T, 0.0), axis=1, keepdims=True)
        source = jnp.floor(mine * (1.0 / TOK))

        def before(i, total):
            columns = pl.ds(pl.multiple_of(i * 512, 512), 512)
            return total + jnp.sum(
                jnp.where(spots_f[:, columns] < source * TOK, 1.0, 0.0), axis=1, keepdims=True
            )

        starts = lax.fori_loop(0, CHOSEN // 512, before, jnp.zeros((ROWS, 1), F32))
        my_rank = lax.broadcasted_iota(jnp.int32, (ROWS, 1), 0).astype(F32) * SEQ + me.astype(F32)
        found = source * SLOTS + jnp.floor((my_rank - starts) * (1.0 / SEQ))
        take[...] = jnp.where(
            lax.broadcasted_iota(jnp.int32, (ROWS, MOST), 1).astype(F32) == found, 1.0, 0.0
        ).astype(BF16)

    def bias_blocks(low, high):
        for slot in range(low, high):
            spots = jnp.where(
                lax.broadcasted_iota(jnp.int32, (1, ROWS), 1) < SIDE,
                c2t[pl.ds(zf(z_blocks[slot]), 1), :],
                c2t[pl.ds(xf(x_blocks[slot]), 1), :],
            )
            bias[:, slot * ROWS : (slot + 1) * ROWS] = jnp.where(
                spots <= cpos[0, :, 0:1], 0.0, FAR
            )

    work = [functools.partial(gather_rows, n) for n in range(D // 256)]
    work += [functools.partial(normalize, n) for n in range(D // 512)]
    work += [dealt_order, place_rows, find_slots]
    work += [functools.partial(bias_blocks, n, n + 4) for n in range(0, SEQ, 4)]

    w_steps[0]()
    token_load.wait()
    done = 0
    for i in range(1, len(w_steps)):
        until = len(work) * i // (len(w_steps) - 1)
        for item in work[done:until]:
            item()
        done = until
        w_steps[i]()
        if i == NZ - 1:
            o_steps[0]()
        if i >= NZ + 1 and i - NZ < NZ:
            o_steps[i - NZ]()

    def part(a, k, low=0, high=SEQ):
        return wqo.at[a, pl.ds(low, high - low), along_y(k)]

    def along(a, k, slot, to, low=0, high=SEQ):
        return remote(
            part(a, k, low, high), part(a, k, low, high), y_send, y_recv.at[a, slot], along_y(to), me
        )

    def across(a, k):
        remote(part(a, k), part(a, k), p_send, p_recv.at[a], partner, me).start()

    def y_first(a):
        along(a, 0, 0, 1).start()
        along(a, 0, 1, -1).start()
        across(a, 0)

    def y_second(a):
        along(a, -1, 0, 1).wait_recv()
        along(a, -1, 2, 1, 0, SEQ // 2).start()
        across(a, -1)
        along(a, 1, 1, -1).wait_recv()
        along(a, 1, 3, -1, SEQ // 2, SEQ).start()
        across(a, 1)

    def y_third(a):
        along(a, 2, 2, 1, 0, SEQ // 2).wait_recv()
        along(a, 2, 3, -1, SEQ // 2, SEQ).wait_recv()
        across(a, 2)

    def y_last(a):
        whole = wqo.at[a, :, pl.ds(0, 4)]
        pltpu.make_async_copy(whole, whole, p_recv.at[a]).wait()

    whole = kvw.at[pl.ds(0, HALF * SEQ), :]
    pltpu.make_async_copy(whole, whole, d_recv).wait()

    for n in range(2):
        columns = slice(n * 256, (n + 1) * 256)
        kv_own[:, columns] = jnp.dot(
            normed[...], kvw[:, columns], preferred_element_type=F32
        ).astype(BF16)
    leaving = jnp.dot(deal[...], kv_own[...], preferred_element_type=F32)
    kv_slots[...] = leaving.reshape(SEQ, SLOTS, 2 * KW).astype(BF16)

    def send_slot(j, carry):
        dest = lax.rem(me + j, SEQ)
        remote(kv_slots.at[dest], kv_in.at[me], a_send, a_recv, dp, dest).start()
        return carry

    lax.fori_loop(1, SEQ, send_slot, 0)
    kv_in[me] = kv_slots[me]

    for i in range(NZ, len(o_steps)):
        o_steps[i]()
    for i in range(EARLY):
        from_y(i)

    whole = kv_in.at[pl.ds(0, SEQ - 1)]
    pltpu.make_async_copy(whole, whole, a_recv).wait()
    came = kv_in[...].astype(F32).reshape(MOST, 2 * KW).astype(BF16)
    kv[0:ROWS, :] = jnp.dot(take[...], came, preferred_element_type=F32).astype(BF16)

    def second_gather(route, at, na, nb, order):
        groups = ring_groups(na, nb)[0]

        def rows(n):
            return kv.at[pl.ds(n * ROWS + route * SIDE, SIDE), :]

        def send(block, to):
            n = order[block[0] % na, block[1] % nb][0]
            lands, group = order[(block[0] - to[0]) % na, (block[1] - to[1]) % nb]
            remote(rows(n), rows(lands), kv_send, kv_recv.at[route, group], dp, at(to)).start()

        def wait(index):
            some = kv.at[pl.ds(0, len(groups[index]) * SIDE), :]
            pltpu.make_async_copy(some, some, kv_recv.at[route, index]).wait()

        return ring_steps(na, nb, False, send, wait)

    z_steps = second_gather(0, zf, NZ, NX, z_places)
    x_steps = second_gather(1, xf, NX, NZ, x_places)

    def attend(g, pair):
        e = pair // (GROUP // PAIR)
        rows = slice(g * CHUNK, (g + 1) * CHUNK)
        keys = kv[rows, pl.ds(pl.multiple_of(e * HEAD_DIM, HEAD_DIM), HEAD_DIM)]
        values = kv[rows, pl.ds(pl.multiple_of(KW + e * HEAD_DIM, HEAD_DIM), HEAD_DIM)]
        heads = [pair * PAIR + n for n in range(PAIR)]
        columns = [pl.ds(pl.multiple_of(h * HEAD_DIM, HEAD_DIM), HEAD_DIM) for h in heads]
        scores = [
            lax.dot_general(
                query[:, c], keys, (((1,), (1,)), ((), ())), preferred_element_type=F32
            )
            for c in columns
        ]
        for h, c, score in zip(heads, columns, scores):
            score = score + bias[:, rows]
            fresh = jnp.max(score, axis=1, keepdims=True)
            if g > 0:
                before = top_ref[h][:, 0:1]
                fresh = jnp.maximum(before, fresh)
            probs = jnp.exp(score - fresh)
            total = jnp.sum(probs, axis=1, keepdims=True)
            acc = jnp.dot(probs.astype(BF16), values, preferred_element_type=F32)
            if g > 0:
                shrink = jnp.exp(before - fresh)
                total = total_ref[h][:, 0:1] * shrink + total
                acc = acc_ref[h] * shrink + acc
            if g < CHOSEN // CHUNK - 1:
                top_ref[h] = jnp.broadcast_to(fresh, (MOST, 128))
                total_ref[h] = jnp.broadcast_to(total, (MOST, 128))
                acc_ref[h] = acc
            else:
                att[:, c] = (acc / total).astype(BF16)

    def project_q():
        def tile(n, carry):
            columns = pl.ds(pl.multiple_of(n * 256, 256), 256)
            weights = wqo[0, :, :, :, columns].reshape(D, 256)
            piece = jnp.dot(normed[...], weights, preferred_element_type=F32)
            query[:, columns] = (piece * HEAD_DIM ** (-0.5)).astype(BF16)
            return carry

        lax.fori_loop(0, QW // 256, tile, 0)

    def last_of_y():
        y_first(1)
        whole = wqo.at[0, :, 0]
        pltpu.make_async_copy(whole, whole, q_recv.at[SEQ // 2]).wait()
        across(0, 2)

    z_steps[0]()
    x_steps[0]()
    for i in range(EARLY, SEQ // 2):
        from_y(i)
        if i == 9:
            z_steps[1]()
            x_steps[1]()
            z_steps[2]()
            x_steps[2]()
        if i == 14:
            x_steps[3]()
            z_steps[3]()
            z_steps[4]()
    last_of_y()
    x_steps[4]()
    z_steps[5]()
    z_steps[6]()
    y_last(0)
    project_q()
    x_steps[5]()
    z_steps[7]()

    windows = {
        1: [[z_steps[n + 8], x_steps[n + 6]] for n in range(4)],
        2: [[z_steps[n + 12], x_steps[n + 10]] for n in range(4)],
        3: [[x_steps[14]], [x_steps[15]], [z_steps[16]], [x_steps[16]]],
    }
    for g in range(1, CHOSEN // CHUNK):
        if g == 3:
            y_second(1)

        def together(i, carry):
            for j in range(HEADS // PAIR):

                @pl.when(i == j)
                def _():
                    for step in windows[g][j]:
                        step()

            attend(g - 1, i)
            return carry

        lax.fori_loop(0, HEADS // PAIR, together, 0)

    def alone(i, carry):
        attend(CHOSEN // CHUNK - 1, i)
        return carry

    lax.fori_loop(0, HEADS // PAIR, alone, 0)
    y_third(1)
    y_last(1)

    def project_out(n, carry):
        columns = pl.ds(pl.multiple_of(n * 256, 256), 256)
        weights = wqo[1, pl.ds(n * 4, 4)].reshape(256, QW)
        out_tile[n] = lax.dot_general(
            att[...], weights, (((1,), (1,)), ((), ())), preferred_element_type=F32
        ).astype(BF16)
        pltpu.make_async_copy(out_tile.at[n], out.at[n], out_sem.at[0]).start()
        return carry

    meta_copy = pltpu.make_async_copy(meta, meta_out, out_sem.at[1])
    meta_copy.start()
    lax.fori_loop(0, D // 256, project_out, 0)

    for whole, sem in (
        (kvw.at[pl.ds(0, HALF * (SEQ - 1)), :], w_send),
        (kvw.at[pl.ds(0, HALF * SEQ), :], d_send),
        (wqo.at[:, pl.ds(0, SEQ - 1), 0], o_send),
        (kv_in.at[pl.ds(0, SEQ - 1)], a_send),
        (kv.at[pl.ds(0, ROWS * (SEQ - 1)), :], kv_send),
        (wqo.at[0, :, pl.ds(0, 3)], q_send),
        (wqo.at[1, :, pl.ds(0, 3)], y_send),
        (wqo.at[:, :, pl.ds(0, 4)], p_send),
    ):
        pltpu.make_async_copy(whole, whole, sem).wait()
    meta_copy.wait()
    pltpu.make_async_copy(out_tile, out, out_sem.at[0]).wait()


def mix_kernel(tokens, block_out, meta, mixed, tok, rows_in, result, load_sem, rows_sem, store_sem):
    def load(n):
        return pltpu.make_async_copy(tokens.at[n], tok.at[n], load_sem.at[n])

    def store(n):
        return pltpu.make_async_copy(result.at[n], mixed.at[n], store_sem.at[n])

    rows_load = pltpu.make_async_copy(block_out, rows_in, rows_sem)
    rows_load.start()
    for n in range(TILES):
        load(n).start()
    rows_load.wait()

    def tile(n, carry):
        place = lax.broadcasted_iota(jnp.int32, (TILE, MOST), 0) + n * TILE
        hit = place.astype(F32) == meta[0:1, :]
        high = meta[1:2, :].astype(BF16).astype(F32)
        low = meta[1:2, :] - high
        lift_high = jnp.where(hit, high, 0.0).astype(BF16)
        lift_low = jnp.where(hit, low, 0.0).astype(BF16)
        load(n).wait()
        for c in range(D // 256):
            columns = slice(c * 256, (c + 1) * 256)
            rows = jnp.dot(lift_high, rows_in[c], preferred_element_type=F32)
            rows = rows + jnp.dot(lift_low, rows_in[c], preferred_element_type=F32)
            result[n, :, columns] = (tok[n, :, columns].astype(F32) + rows).astype(BF16)
        store(n).start()
        return carry

    lax.fori_loop(0, TILES, tile, 0)
    for n in range(TILES):
        store(n).wait()


def per_device(tokens, chosen, gates, w_query, w_key, w_value, w_out):
    anywhere = pl.BlockSpec(memory_space=pl.ANY)
    inside = pl.BlockSpec(memory_space=pltpu.VMEM)
    dma = pltpu.SemaphoreType.DMA
    vmem = pltpu.VMEM
    block_out, meta = pl.pallas_call(
        block_kernel,
        out_shape=(
            jax.ShapeDtypeStruct((D // 256, MOST, 256), BF16),
            jax.ShapeDtypeStruct((8, MOST), F32),
        ),
        in_specs=[anywhere] * 5 + [inside] * 3,
        out_specs=(anywhere, anywhere),
        scratch_shapes=[
            vmem((D // 256, MOST, 256), BF16),
            vmem((8, MOST), F32),
            vmem((TOK, D), BF16),
            vmem((D, 2 * KW), BF16),
            vmem((2, SEQ, PARTS, PIECE, QW), BF16),
            vmem((MOST, D), BF16),
            vmem((MOST, TOK), BF16),
            vmem((MOST, MOST), BF16),
            vmem((ROWS, MOST), BF16),
            vmem((MOST, CHOSEN), F32),
            vmem((MOST, QW), BF16),
            vmem((MOST, QW), BF16),
            vmem((MOST, 2 * KW), BF16),
            vmem((SEQ, SLOTS, 2 * KW), BF16),
            vmem((SEQ, SLOTS, 2 * KW), BF16),
            vmem((CHOSEN, 2 * KW), BF16),
            vmem((2, MOST, 128), F32),
            vmem((1, CHOSEN), F32),
            vmem((SEQ, ROWS), F32),
            vmem((MOST, 128), F32),
            vmem((HEADS, MOST, 128), F32),
            vmem((HEADS, MOST, 128), F32),
            vmem((HEADS, MOST, 128), F32),
            dma((4,)),
            dma,
            dma((2,)),
            dma,
            dma((17,)),
            dma,
            dma((17,)),
            dma,
            dma,
            dma,
            dma,
            dma,
            dma((2, 17)),
            dma,
            dma((17,)),
            dma,
            dma((2, 4)),
            dma,
            dma((2,)),
        ],
        compiler_params=pltpu.CompilerParams(
            collective_id=0, has_side_effects=True, vmem_limit_bytes=56 * 1024 * 1024
        ),
        name="block",
    )(
        tokens,
        w_query.reshape(PARTS, PIECE, QW),
        w_key,
        w_value,
        w_out.T.reshape(PARTS, PIECE, QW),
        chosen.reshape(1, CHOSEN),
        gates.reshape(1, CHOSEN),
        chosen.reshape(SEQ, ROWS),
    )
    mixed = pl.pallas_call(
        mix_kernel,
        out_shape=jax.ShapeDtypeStruct((TILES, TILE, D), BF16),
        in_specs=[anywhere, anywhere, inside],
        out_specs=anywhere,
        scratch_shapes=[
            vmem((TILES, TILE, D), BF16),
            vmem((D // 256, MOST, 256), BF16),
            vmem((TILES, TILE, D), BF16),
            dma((TILES,)),
            dma,
            dma((TILES,)),
        ],
        compiler_params=pltpu.CompilerParams(vmem_limit_bytes=56 * 1024 * 1024),
        name="mix",
    )(tokens.reshape(TILES, TILE, D), block_out, meta)
    return mixed.reshape(TOK, D)


def solution(mesh):
    return jax.shard_map(
        per_device,
        mesh=mesh,
        in_specs=(
            P(("dp", "seq"), None),
            P("dp"),
            P("dp"),
            P("seq", None),
            P("seq", None),
            P("seq", None),
            P(None, "seq"),
        ),
        out_specs=P(("dp", "seq"), None),
        check_vma=False,
    )
```

```python
import functools

import jax
import jax.numpy as jnp
from jax import lax
from jax.experimental import pallas as pl
from jax.experimental.pallas import tpu as pltpu
from jax.sharding import PartitionSpec as P

HEADS = 8
KV_HEADS = 2
GROUP = HEADS // KV_HEADS
HEAD_DIM = 128
D = 2048
QW = HEADS * HEAD_DIM
KW = KV_HEADS * HEAD_DIM
SEQ = 32
NX = 4
NZ = 8
TOK = 1024
CHOSEN = 4096
ROWS = 128
MOST = 256
SLOTS = 8
DEPTH = D // SEQ
HALF = DEPTH // 2
PARTS = 8
PIECE = DEPTH // PARTS
CHUNK = 1024
PER = CHUNK // ROWS
SIDE = ROWS // 2
EARLY = 5
PAIR = 2
TILE = 256
TILES = TOK // TILE
MESH = pl.DeviceIdType.MESH
F32 = jnp.float32
BF16 = jnp.bfloat16
FAR = -1e30


def ring_groups(na, nb):
    columns = [0]
    for k in range(1, na // 2 + 1):
        columns += [-k, k] if k < na // 2 else [-k]
    groups = [[(0, 0)]] + [[(j, 0)] for j in columns[1:]]
    for m in range(1, nb // 2):
        groups += [[(j, -m), (j, m)] for j in columns]
    return groups + [[(j, far_side(n) * -(nb // 2)) for n, j in enumerate(columns)]], columns


def far_side(order):
    return 1 if order % 2 == 0 else -1


def ring_steps(na, nb, direct, far, send, wait):
    groups, columns = ring_groups(na, nb)
    across = [(0, 1), (0, -1)] + ([(0, m) for m in range(2, nb - 1)] if far else [])

    def first():
        along = [(-p, 0) for p in columns[1:]] if direct else [(1, 0), (-1, 0)]
        for to in along + across:
            send((0, 0), to)

    def step(index):
        wait(index)
        for j, m in groups[index]:
            if m == 0:
                side = -1 if j > 0 else 1
                if not direct and abs(j) < (na // 2 if side == 1 else na // 2 - 1):
                    send((j, m), (side, 0))
                for to in across:
                    send((j, m), to)
            elif not far:
                side = -1 if m > 0 else 1
                reach = nb // 2 if side == far_side(columns.index(j)) else nb // 2 - 1
                if abs(m) < reach:
                    send((j, m), (0, side))

    return [first] + [functools.partial(step, n) for n in range(1, len(groups))]


def places(na, nb):
    flat = {}
    for index, group in enumerate(ring_groups(na, nb)[0]):
        for j, m in group:
            flat[j % na, m % nb] = (len(flat), index)
    return flat


def block_kernel(
    tokens, wq, wk, wv, wo, crow, grow, listed_in,
    out, meta_out,
    out_tile, meta, tok, kvw, wqo, normed, onehot, deal, take, bias, query, att, kv_own, kv_slots, kv_in, kv,
    cpos, spots_f, c2t, wide, top_ref, total_ref, acc_ref,
    load_sem, tok_sem, out_sem, w_send, w_recv, o_send, o_recv, d_send, d_recv, a_send, a_recv,
    kv_send, kv_recv, q_send, q_recv, y_send, y_recv, p_send, p_recv,
):
    dp = lax.axis_index("dp")
    me = lax.axis_index("seq")
    core = lax.rem(dp, 2)
    y = dp // 2
    partner = dp + 1 - 2 * core
    x, z = me // NZ, lax.rem(me, NZ)

    def along_y(k):
        return lax.rem(y + k + 4, 4) * 2 + core

    def zf(block):
        return lax.rem(x + block[1] + NX, NX) * NZ + lax.rem(z + block[0] + NZ, NZ)

    def xf(block):
        return lax.rem(x + block[0] + NX, NX) * NZ + lax.rem(z + block[1] + NZ, NZ)

    def remote(src, dst, send_sem, recv_sem, to_dp, to_seq):
        return pltpu.make_async_remote_copy(
            src_ref=src,
            dst_ref=dst,
            send_sem=send_sem,
            recv_sem=recv_sem,
            device_id=(to_dp, to_seq),
            device_id_type=MESH,
        )

    def kv_unit(s, half):
        start = s * DEPTH + half * HALF
        return pl.ds(pl.multiple_of(start, HALF), HALF)

    own = kv_unit(me, core)
    loads = [
        pltpu.make_async_copy(wk.at[pl.ds(core * HALF, HALF), :], kvw.at[own, 0:KW], load_sem.at[0]),
        pltpu.make_async_copy(wv.at[pl.ds(core * HALF, HALF), :], kvw.at[own, KW : 2 * KW], load_sem.at[1]),
        pltpu.make_async_copy(wq.at[dp], wqo.at[0, me, dp], load_sem.at[2]),
        pltpu.make_async_copy(wo.at[dp], wqo.at[1, me, dp], load_sem.at[3]),
    ]
    for copy in loads:
        copy.start()
    token_load = pltpu.make_async_copy(tokens, tok, tok_sem)
    token_load.start()

    barrier = pltpu.get_barrier_semaphore()

    def greet(j, carry):
        pl.semaphore_signal(
            barrier, inc=1, device_id=(dp, lax.rem(me + j, SEQ)), device_id_type=MESH
        )
        return carry

    lax.fori_loop(1, SEQ, greet, 0)
    for other in (partner, along_y(1), along_y(-1)):
        pl.semaphore_signal(barrier, inc=1, device_id=(other, me), device_id_type=MESH)

    base = (me * TOK).astype(F32)
    listed = crow[...].astype(F32)
    spots_f[...] = listed
    first = jnp.sum(jnp.where(listed < base, 1.0, 0.0), axis=1, keepdims=True)
    last = jnp.sum(jnp.where(listed < base + TOK, 1.0, 0.0), axis=1, keepdims=True)
    shift = jnp.minimum(first, float(CHOSEN - MOST))

    def pick(i, carry):
        rows = pl.ds(pl.multiple_of(i * 32, 32), 32)
        lane = lax.broadcasted_iota(jnp.int32, (32, CHOSEN), 1).astype(F32)
        rank = lax.broadcasted_iota(jnp.int32, (32, 1), 0).astype(F32)
        hit = lane == rank + (shift + (i * 32).astype(F32))
        spot = jnp.sum(jnp.where(hit, spots_f[...], 0.0), axis=1, keepdims=True)
        gate = jnp.sum(jnp.where(hit, grow[...], 0.0), axis=1, keepdims=True)
        cpos[0, rows, :] = jnp.broadcast_to(spot, (32, 128))
        cpos[1, rows, :] = jnp.broadcast_to(gate, (32, 128))
        return carry

    lax.fori_loop(0, MOST // 32, pick, 0)
    place = lax.broadcasted_iota(jnp.int32, (MOST, TOK), 1).astype(F32)
    onehot[...] = jnp.where(place == cpos[0, :, 0:1] - base, 1.0, 0.0).astype(BF16)

    for copy in loads:
        copy.wait()
    pl.semaphore_wait(barrier, SEQ + 2)

    z_places, x_places = places(NZ, NX), places(NX, NZ)
    z_blocks, x_blocks = list(z_places), list(x_places)

    def block_at(i):
        return zf(z_blocks[i])

    def q_copy(s, k, sem, to):
        piece = wqo.at[0, s, along_y(k)]
        return remote(piece, piece, q_send, q_recv.at[sem], along_y(to), me)

    def to_y(n):
        s = block_at(n)
        q_copy(s, 0, n // 2, 1).start()
        q_copy(s, 0, n // 2, -1).start()
        q_across(s, 0)

    def q_across(s, k):
        piece = wqo.at[0, s, along_y(k)]
        remote(piece, piece, p_send, p_recv.at[0], partner, me).start()

    def from_y(i):
        both = wqo.at[0, pl.ds(0, 4), 0]
        pltpu.make_async_copy(both, both, q_recv.at[i]).wait()
        low, high = block_at(2 * i), block_at(2 * i + 1)
        q_copy(low, -1, SEQ // 2, 1).start()
        q_copy(high, 1, SEQ // 2, -1).start()
        for s in (low, high):
            q_across(s, -1)
            q_across(s, 1)

    def first_gather(far, view, many, send_sem, recv_sem, arrived):
        groups = ring_groups(NZ, NX)[0]

        def send(block, to):
            group = z_places[(block[0] - to[0]) % NZ, (block[1] - to[1]) % NX][1]
            s = zf(block)
            remote(view(s), view(s), send_sem, recv_sem.at[group], dp, zf(to)).start()

        def wait(index):
            some = many(len(groups[index]))
            pltpu.make_async_copy(some, some, recv_sem.at[index]).wait()

        def then(index, step):
            step()
            for block in groups[index]:
                arrived(z_places[block[0] % NZ, block[1] % NX][0])

        steps = ring_steps(NZ, NX, True, far, send, wait)
        return [functools.partial(then, index, step) for index, step in enumerate(steps)]

    def kv_half(s):
        return kvw.at[kv_unit(s, core), :]

    def to_partner(n):
        half = kv_half(block_at(n))
        remote(half, half, d_send, d_recv, partner, me).start()

    w_steps = first_gather(
        False,
        kv_half, lambda n: kvw.at[pl.ds(0, n * HALF), :], w_send, w_recv, to_partner,
    )
    q_steps = first_gather(
        True,
        lambda s: wqo.at[0, s, dp], lambda n: wqo.at[0, pl.ds(0, n), 0],
        o_send.at[0], o_recv.at[0], to_y,
    )
    o_steps = first_gather(
        True,
        lambda s: wqo.at[1, s, dp], lambda n: wqo.at[1, pl.ds(0, n), 0],
        o_send.at[1], o_recv.at[1], lambda n: None,
    )

    def gather_rows(n):
        columns = slice(n * 256, (n + 1) * 256)
        part = jnp.dot(onehot[...], tok[:, columns], preferred_element_type=F32)
        normed[:, columns] = part.astype(BF16)
        square = jnp.broadcast_to(jnp.sum(part * part, axis=1, keepdims=True), (MOST, 128))
        wide[...] = square if n == 0 else wide[...] + square

    def normalize(n):
        columns = slice(n * 512, (n + 1) * 512)
        scale = lax.rsqrt(wide[:, 0:1] * (1.0 / D) + 1e-06)
        normed[:, columns] = (normed[:, columns].astype(F32) * scale).astype(BF16)

    def place_rows():
        order = lax.broadcasted_iota(jnp.int32, (MOST, MOST), 1)
        slot = lax.broadcasted_iota(jnp.int32, (MOST, MOST), 0)
        rank = order + shift.astype(jnp.int32)
        offset = rank - first.astype(jnp.int32)
        inside = jnp.where(offset >= 0, 1, 0) * jnp.where(rank < last.astype(jnp.int32), 1, 0)
        goes = (rank & (SEQ - 1)) * SLOTS + (offset >> 5)
        deal[...] = jnp.where(goes == slot, inside, 0).astype(F32).astype(BF16)
        gate = cpos[1, :, 0:1]
        eye = order == slot
        meta[0:1, :] = jnp.sum(jnp.where(eye, cpos[0, :, 0:1] - base, 0.0), axis=0, keepdims=True)
        meta[1:2, :] = jnp.sum(jnp.where(eye, gate, 0.0), axis=0, keepdims=True)

    def dealt_order():
        rows = listed_in[...].astype(F32)
        r = lax.broadcasted_iota(jnp.int32, (SEQ, ROWS), 0)
        k = lax.broadcasted_iota(jnp.int32, (SEQ, ROWS), 1)
        for q in range(ROWS // SEQ):
            take_k = jnp.where(k == r * (ROWS // SEQ) + q, 1.0, 0.0)
            part = lax.dot_general(
                rows[:, q * SEQ : (q + 1) * SEQ], take_k, (((0,), (0,)), ((), ())),
                precision=lax.Precision.HIGHEST, preferred_element_type=F32,
            )
            c2t[...] = part if q == 0 else c2t[...] + part

    def find_slots():
        lane32 = lax.broadcasted_iota(jnp.int32, (ROWS, SEQ), 1)
        mine = jnp.sum(jnp.where(lane32 == me, c2t[...].T, 0.0), axis=1, keepdims=True)
        source = jnp.floor(mine * (1.0 / TOK))

        def before(i, total):
            columns = pl.ds(pl.multiple_of(i * 512, 512), 512)
            return total + jnp.sum(
                jnp.where(spots_f[:, columns] < source * TOK, 1.0, 0.0), axis=1, keepdims=True
            )

        starts = lax.fori_loop(0, CHOSEN // 512, before, jnp.zeros((ROWS, 1), F32))
        my_rank = lax.broadcasted_iota(jnp.int32, (ROWS, 1), 0).astype(F32) * SEQ + me.astype(F32)
        found = source * SLOTS + jnp.floor((my_rank - starts) * (1.0 / SEQ))
        take[...] = jnp.where(
            lax.broadcasted_iota(jnp.int32, (ROWS, MOST), 1).astype(F32) == found, 1.0, 0.0
        ).astype(BF16)

    def bias_blocks(low, high):
        for slot in range(low, high):
            spots = jnp.where(
                lax.broadcasted_iota(jnp.int32, (1, ROWS), 1) < SIDE,
                c2t[pl.ds(zf(z_blocks[slot]), 1), :],
                c2t[pl.ds(xf(x_blocks[slot]), 1), :],
            )
            bias[:, slot * ROWS : (slot + 1) * ROWS] = jnp.where(
                spots <= cpos[0, :, 0:1], 0.0, FAR
            )

    work = [functools.partial(gather_rows, n) for n in range(D // 256)]
    work += [functools.partial(normalize, n) for n in range(D // 512)]
    work += [dealt_order, place_rows, find_slots]
    work += [functools.partial(bias_blocks, n, n + 4) for n in range(0, SEQ, 4)]

    w_steps[0]()
    token_load.wait()
    done = 0
    for i in range(1, len(w_steps)):
        until = len(work) * i // (len(w_steps) - 1)
        for item in work[done:until]:
            item()
        done = until
        w_steps[i]()
        if i == NZ - 1:
            q_steps[0]()
            o_steps[0]()

    for n in range(1, NZ):
        q_steps[n]()
    for n in range(1, NZ):
        o_steps[n]()

    def part(a, k, low=0, high=SEQ):
        return wqo.at[a, pl.ds(low, high - low), along_y(k)]

    def along(a, k, slot, to, low=0, high=SEQ):
        return remote(
            part(a, k, low, high), part(a, k, low, high), y_send, y_recv.at[a, slot], along_y(to), me
        )

    def across(a, k):
        remote(part(a, k), part(a, k), p_send, p_recv.at[a], partner, me).start()

    def y_first(a):
        along(a, 0, 0, 1).start()
        along(a, 0, 1, -1).start()
        across(a, 0)

    def y_second(a):
        along(a, -1, 0, 1).wait_recv()
        along(a, -1, 2, 1, 0, SEQ // 2).start()
        across(a, -1)
        along(a, 1, 1, -1).wait_recv()
        along(a, 1, 3, -1, SEQ // 2, SEQ).start()
        across(a, 1)

    def y_third(a):
        along(a, 2, 2, 1, 0, SEQ // 2).wait_recv()
        along(a, 2, 3, -1, SEQ // 2, SEQ).wait_recv()
        across(a, 2)

    def y_last(a):
        whole = wqo.at[a, :, pl.ds(0, 4)]
        pltpu.make_async_copy(whole, whole, p_recv.at[a]).wait()

    whole = kvw.at[pl.ds(0, HALF * SEQ), :]
    pltpu.make_async_copy(whole, whole, d_recv).wait()

    for n in range(2):
        columns = slice(n * 256, (n + 1) * 256)
        kv_own[:, columns] = jnp.dot(
            normed[...], kvw[:, columns], preferred_element_type=F32
        ).astype(BF16)
    leaving = jnp.dot(deal[...], kv_own[...], preferred_element_type=F32)
    kv_slots[...] = leaving.reshape(SEQ, SLOTS, 2 * KW).astype(BF16)

    def send_slot(j, carry):
        dest = lax.rem(me + j, SEQ)
        remote(kv_slots.at[dest], kv_in.at[me], a_send, a_recv, dp, dest).start()
        return carry

    lax.fori_loop(1, SEQ, send_slot, 0)
    kv_in[me] = kv_slots[me]

    for i in range(NZ, len(q_steps)):
        q_steps[i]()
    for i in range(EARLY):
        from_y(i)

    whole = kv_in.at[pl.ds(0, SEQ - 1)]
    pltpu.make_async_copy(whole, whole, a_recv).wait()
    came = kv_in[...].astype(F32).reshape(MOST, 2 * KW).astype(BF16)
    kv[0:ROWS, :] = jnp.dot(take[...], came, preferred_element_type=F32).astype(BF16)

    def second_gather(route, at, na, nb, order):
        groups = ring_groups(na, nb)[0]

        def rows(n):
            return kv.at[pl.ds(n * ROWS + route * SIDE, SIDE), :]

        def send(block, to):
            n = order[block[0] % na, block[1] % nb][0]
            lands, group = order[(block[0] - to[0]) % na, (block[1] - to[1]) % nb]
            remote(rows(n), rows(lands), kv_send, kv_recv.at[route, group], dp, at(to)).start()

        def wait(index):
            some = kv.at[pl.ds(0, len(groups[index]) * SIDE), :]
            pltpu.make_async_copy(some, some, kv_recv.at[route, index]).wait()

        return ring_steps(na, nb, False, False, send, wait)

    z_steps = second_gather(0, zf, NZ, NX, z_places)
    x_steps = second_gather(1, xf, NX, NZ, x_places)

    def attend(g, pair):
        e = pair // (GROUP // PAIR)
        rows = slice(g * CHUNK, (g + 1) * CHUNK)
        keys = kv[rows, pl.ds(pl.multiple_of(e * HEAD_DIM, HEAD_DIM), HEAD_DIM)]
        values = kv[rows, pl.ds(pl.multiple_of(KW + e * HEAD_DIM, HEAD_DIM), HEAD_DIM)]
        heads = [pair * PAIR + n for n in range(PAIR)]
        columns = [pl.ds(pl.multiple_of(h * HEAD_DIM, HEAD_DIM), HEAD_DIM) for h in heads]
        scores = [
            lax.dot_general(
                query[:, c], keys, (((1,), (1,)), ((), ())), preferred_element_type=F32
            )
            for c in columns
        ]
        for h, c, score in zip(heads, columns, scores):
            score = score + bias[:, rows]
            fresh = jnp.max(score, axis=1, keepdims=True)
            if g > 0:
                before = top_ref[h][:, 0:1]
                fresh = jnp.maximum(before, fresh)
            probs = jnp.exp(score - fresh)
            total = jnp.sum(probs, axis=1, keepdims=True)
            acc = jnp.dot(probs.astype(BF16), values, preferred_element_type=F32)
            if g > 0:
                shrink = jnp.exp(before - fresh)
                total = total_ref[h][:, 0:1] * shrink + total
                acc = acc_ref[h] * shrink + acc
            if g < CHOSEN // CHUNK - 1:
                top_ref[h] = jnp.broadcast_to(fresh, (MOST, 128))
                total_ref[h] = jnp.broadcast_to(total, (MOST, 128))
                acc_ref[h] = acc
            else:
                att[:, c] = (acc / total).astype(BF16)

    def project_q():
        def tile(n, carry):
            columns = pl.ds(pl.multiple_of(n * 256, 256), 256)
            weights = wqo[0, :, :, :, columns].reshape(D, 256)
            piece = jnp.dot(normed[...], weights, preferred_element_type=F32)
            query[:, columns] = (piece * HEAD_DIM ** (-0.5)).astype(BF16)
            return carry

        lax.fori_loop(0, QW // 256, tile, 0)

    def last_of_y():
        y_first(1)
        whole = wqo.at[0, :, 0]
        pltpu.make_async_copy(whole, whole, q_recv.at[SEQ // 2]).wait()
        across(0, 2)

    z_steps[0]()
    x_steps[0]()
    for i in range(EARLY, SEQ // 2):
        from_y(i)
        if i == 9:
            z_steps[1]()
            x_steps[1]()
            z_steps[2]()
            x_steps[2]()
        if i == 14:
            x_steps[3]()
            z_steps[3]()
            z_steps[4]()
    for i in range(NZ, len(o_steps)):
        o_steps[i]()
    x_steps[4]()
    z_steps[5]()
    z_steps[6]()
    last_of_y()
    x_steps[5]()
    y_last(0)
    project_q()
    z_steps[7]()

    windows = {
        1: [[z_steps[n + 8], x_steps[n + 6]] for n in range(4)],
        2: [[z_steps[n + 12], x_steps[n + 10]] for n in range(4)],
        3: [[x_steps[14]], [x_steps[15]], [z_steps[16]], [x_steps[16]]],
    }
    for g in range(1, CHOSEN // CHUNK):
        if g == 3:
            y_second(1)

        def together(i, carry):
            for j in range(HEADS // PAIR):

                @pl.when(i == j)
                def _():
                    for step in windows[g][j]:
                        step()

            attend(g - 1, i)
            return carry

        lax.fori_loop(0, HEADS // PAIR, together, 0)

    def alone(i, carry):
        attend(CHOSEN // CHUNK - 1, i)
        return carry

    lax.fori_loop(0, HEADS // PAIR, alone, 0)
    y_third(1)
    y_last(1)

    def project_out(n, carry):
        columns = pl.ds(pl.multiple_of(n * 256, 256), 256)
        weights = wqo[1, pl.ds(n * 4, 4)].reshape(256, QW)
        out_tile[n] = lax.dot_general(
            att[...], weights, (((1,), (1,)), ((), ())), preferred_element_type=F32
        ).astype(BF16)
        pltpu.make_async_copy(out_tile.at[n], out.at[n], out_sem.at[0]).start()
        return carry

    meta_copy = pltpu.make_async_copy(meta, meta_out, out_sem.at[1])
    meta_copy.start()
    lax.fori_loop(0, D // 256, project_out, 0)

    for whole, sem in (
        (kvw.at[pl.ds(0, HALF * (SEQ - 1)), :], w_send),
        (kvw.at[pl.ds(0, HALF * SEQ), :], d_send),
        (wqo.at[0, pl.ds(0, SEQ - 1), 0], o_send.at[0]),
        (wqo.at[1, pl.ds(0, SEQ - 1), 0], o_send.at[1]),
        (kv_in.at[pl.ds(0, SEQ - 1)], a_send),
        (kv.at[pl.ds(0, ROWS * (SEQ - 1)), :], kv_send),
        (wqo.at[0, :, pl.ds(0, 3)], q_send),
        (wqo.at[1, :, pl.ds(0, 3)], y_send),
        (wqo.at[:, :, pl.ds(0, 4)], p_send),
    ):
        pltpu.make_async_copy(whole, whole, sem).wait()
    meta_copy.wait()
    pltpu.make_async_copy(out_tile, out, out_sem.at[0]).wait()


def mix_kernel(tokens, block_out, meta, mixed, tok, rows_in, result, load_sem, rows_sem, store_sem):
    def load(n):
        return pltpu.make_async_copy(tokens.at[n], tok.at[n], load_sem.at[n])

    def store(n):
        return pltpu.make_async_copy(result.at[n], mixed.at[n], store_sem.at[n])

    rows_load = pltpu.make_async_copy(block_out, rows_in, rows_sem)
    rows_load.start()
    for n in range(TILES):
        load(n).start()
    rows_load.wait()

    def tile(n, carry):
        place = lax.broadcasted_iota(jnp.int32, (TILE, MOST), 0) + n * TILE
        hit = place.astype(F32) == meta[0:1, :]
        gate = jnp.sum(jnp.where(hit, meta[1:2, :], 0.0), axis=1, keepdims=True)
        gate = jnp.broadcast_to(gate, (TILE, 256))
        chosen_row = jnp.where(hit, 1.0, 0.0).astype(BF16)
        load(n).wait()
        for c in range(D // 256):
            columns = slice(c * 256, (c + 1) * 256)
            rows = jnp.dot(chosen_row, rows_in[c], preferred_element_type=F32)
            result[n, :, columns] = (tok[n, :, columns].astype(F32) + gate * rows).astype(BF16)
        store(n).start()
        return carry

    lax.fori_loop(0, TILES, tile, 0)
    for n in range(TILES):
        store(n).wait()


def per_device(tokens, chosen, gates, w_query, w_key, w_value, w_out):
    anywhere = pl.BlockSpec(memory_space=pl.ANY)
    inside = pl.BlockSpec(memory_space=pltpu.VMEM)
    dma = pltpu.SemaphoreType.DMA
    vmem = pltpu.VMEM
    block_out, meta = pl.pallas_call(
        block_kernel,
        out_shape=(
            jax.ShapeDtypeStruct((D // 256, MOST, 256), BF16),
            jax.ShapeDtypeStruct((8, MOST), F32),
        ),
        in_specs=[anywhere] * 5 + [inside] * 3,
        out_specs=(anywhere, anywhere),
        scratch_shapes=[
            vmem((D // 256, MOST, 256), BF16),
            vmem((8, MOST), F32),
            vmem((TOK, D), BF16),
            vmem((D, 2 * KW), BF16),
            vmem((2, SEQ, PARTS, PIECE, QW), BF16),
            vmem((MOST, D), BF16),
            vmem((MOST, TOK), BF16),
            vmem((MOST, MOST), BF16),
            vmem((ROWS, MOST), BF16),
            vmem((MOST, CHOSEN), F32),
            vmem((MOST, QW), BF16),
            vmem((MOST, QW), BF16),
            vmem((MOST, 2 * KW), BF16),
            vmem((SEQ, SLOTS, 2 * KW), BF16),
            vmem((SEQ, SLOTS, 2 * KW), BF16),
            vmem((CHOSEN, 2 * KW), BF16),
            vmem((2, MOST, 128), F32),
            vmem((1, CHOSEN), F32),
            vmem((SEQ, ROWS), F32),
            vmem((MOST, 128), F32),
            vmem((HEADS, MOST, 128), F32),
            vmem((HEADS, MOST, 128), F32),
            vmem((HEADS, MOST, 128), F32),
            dma((4,)),
            dma,
            dma((2,)),
            dma,
            dma((17,)),
            dma((2,)),
            dma((2, 17)),
            dma,
            dma,
            dma,
            dma,
            dma,
            dma((2, 17)),
            dma,
            dma((17,)),
            dma,
            dma((2, 4)),
            dma,
            dma((2,)),
        ],
        compiler_params=pltpu.CompilerParams(
            collective_id=0, has_side_effects=True, vmem_limit_bytes=56 * 1024 * 1024
        ),
        name="block",
    )(
        tokens,
        w_query.reshape(PARTS, PIECE, QW),
        w_key,
        w_value,
        w_out.T.reshape(PARTS, PIECE, QW),
        chosen.reshape(1, CHOSEN),
        gates.reshape(1, CHOSEN),
        chosen.reshape(SEQ, ROWS),
    )
    mixed = pl.pallas_call(
        mix_kernel,
        out_shape=jax.ShapeDtypeStruct((TILES, TILE, D), BF16),
        in_specs=[anywhere, anywhere, inside],
        out_specs=anywhere,
        scratch_shapes=[
            vmem((TILES, TILE, D), BF16),
            vmem((D // 256, MOST, 256), BF16),
            vmem((TILES, TILE, D), BF16),
            dma((TILES,)),
            dma,
            dma((TILES,)),
        ],
        compiler_params=pltpu.CompilerParams(vmem_limit_bytes=56 * 1024 * 1024),
        name="mix",
    )(tokens.reshape(TILES, TILE, D), block_out, meta)
    return mixed.reshape(TOK, D)


def solution(mesh):
    return jax.shard_map(
        per_device,
        mesh=mesh,
        in_specs=(
            P(("dp", "seq"), None),
            P("dp"),
            P("dp"),
            P("seq", None),
            P("seq", None),
            P("seq", None),
            P(None, "seq"),
        ),
        out_specs=P(("dp", "seq"), None),
        check_vma=False,
    )
```

```python
import functools

import jax
import jax.numpy as jnp
from jax import lax
from jax.experimental import pallas as pl
from jax.experimental.pallas import tpu as pltpu
from jax.sharding import PartitionSpec as P

HEADS = 8
KV_HEADS = 2
GROUP = HEADS // KV_HEADS
HEAD_DIM = 128
D = 2048
QW = HEADS * HEAD_DIM
KW = KV_HEADS * HEAD_DIM
SEQ = 32
NX = 4
NZ = 8
TOK = 1024
CHOSEN = 4096
ROWS = 128
MOST = 256
SLOTS = 8
DEPTH = D // SEQ
HALF = DEPTH // 2
PARTS = 8
PIECE = DEPTH // PARTS
CHUNK = 1024
PER = CHUNK // ROWS
SIDE = ROWS // 2
EARLY = 5
PAIR = 4
TILE = 512
TILES = TOK // TILE
MESH = pl.DeviceIdType.MESH
F32 = jnp.float32
BF16 = jnp.bfloat16
FAR = -1e30


def ring_groups(na, nb):
    columns = [0]
    for k in range(1, na // 2 + 1):
        columns += [-k, k] if k < na // 2 else [-k]
    groups = [[(0, 0)]] + [[(j, 0)] for j in columns[1:]]
    for m in range(1, nb // 2):
        groups += [[(j, -m), (j, m)] for j in columns]
    return groups + [[(j, far_side(n) * -(nb // 2)) for n, j in enumerate(columns)]], columns


def far_side(order):
    return 1 if order % 2 == 0 else -1


def ring_steps(na, nb, direct, far, send, wait):
    groups, columns = ring_groups(na, nb)
    across = [(0, 1), (0, -1)] + ([(0, m) for m in range(2, nb - 1)] if far else [])

    def first():
        along = [(-p, 0) for p in columns[1:]] if direct else [(1, 0), (-1, 0)]
        for to in along + across:
            send((0, 0), to)

    def step(index):
        wait(index)
        for j, m in groups[index]:
            if m == 0:
                side = -1 if j > 0 else 1
                if not direct and abs(j) < (na // 2 if side == 1 else na // 2 - 1):
                    send((j, m), (side, 0))
                for to in across:
                    send((j, m), to)
            elif not far:
                side = -1 if m > 0 else 1
                reach = nb // 2 if side == far_side(columns.index(j)) else nb // 2 - 1
                if abs(m) < reach:
                    send((j, m), (0, side))

    return [first] + [functools.partial(step, n) for n in range(1, len(groups))]


def places(na, nb):
    flat = {}
    for index, group in enumerate(ring_groups(na, nb)[0]):
        for j, m in group:
            flat[j % na, m % nb] = (len(flat), index)
    return flat


def block_kernel(
    tokens, wq, wk, wv, wo, crow, grow, listed_in,
    out, meta_out,
    out_tile, meta, tok, kvw, wqo, normed, onehot, deal, take, bias, query, att, kv_own, kv_slots, kv_in, kv,
    cpos, spots_f, c2t, wide, top_ref, total_ref, acc_ref,
    load_sem, tok_sem, out_sem, w_send, w_recv, o_send, o_recv, d_send, d_recv, a_send, a_recv,
    kv_send, kv_recv, q_send, q_recv, y_send, y_recv, p_send, p_recv,
):
    dp = lax.axis_index("dp")
    me = lax.axis_index("seq")
    core = lax.rem(dp, 2)
    y = dp // 2
    partner = dp + 1 - 2 * core
    x, z = me // NZ, lax.rem(me, NZ)

    def along_y(k):
        return lax.rem(y + k + 4, 4) * 2 + core

    def zf(block):
        return lax.rem(x + block[1] + NX, NX) * NZ + lax.rem(z + block[0] + NZ, NZ)

    def xf(block):
        return lax.rem(x + block[0] + NX, NX) * NZ + lax.rem(z + block[1] + NZ, NZ)

    def remote(src, dst, send_sem, recv_sem, to_dp, to_seq):
        return pltpu.make_async_remote_copy(
            src_ref=src,
            dst_ref=dst,
            send_sem=send_sem,
            recv_sem=recv_sem,
            device_id=(to_dp, to_seq),
            device_id_type=MESH,
        )

    def kv_unit(s, half):
        start = s * DEPTH + half * HALF
        return pl.ds(pl.multiple_of(start, HALF), HALF)

    own = kv_unit(me, core)
    loads = [
        pltpu.make_async_copy(wk.at[pl.ds(core * HALF, HALF), :], kvw.at[own, 0:KW], load_sem.at[0]),
        pltpu.make_async_copy(wv.at[pl.ds(core * HALF, HALF), :], kvw.at[own, KW : 2 * KW], load_sem.at[1]),
        pltpu.make_async_copy(wq.at[dp], wqo.at[0, me, dp], load_sem.at[2]),
        pltpu.make_async_copy(wo.at[dp], wqo.at[1, me, dp], load_sem.at[3]),
    ]
    for copy in loads:
        copy.start()
    token_load = pltpu.make_async_copy(tokens, tok, tok_sem)
    token_load.start()

    barrier = pltpu.get_barrier_semaphore()

    def greet(j, carry):
        pl.semaphore_signal(
            barrier, inc=1, device_id=(dp, lax.rem(me + j, SEQ)), device_id_type=MESH
        )
        return carry

    lax.fori_loop(1, SEQ, greet, 0)
    for other in (partner, along_y(1), along_y(-1)):
        pl.semaphore_signal(barrier, inc=1, device_id=(other, me), device_id_type=MESH)

    base = (me * TOK).astype(F32)
    listed = crow[...].astype(F32)
    spots_f[...] = listed
    first = jnp.sum(jnp.where(listed < base, 1.0, 0.0), axis=1, keepdims=True)
    last = jnp.sum(jnp.where(listed < base + TOK, 1.0, 0.0), axis=1, keepdims=True)
    shift = jnp.minimum(first, float(CHOSEN - MOST))

    def pick(i, carry):
        rows = pl.ds(pl.multiple_of(i * 32, 32), 32)
        lane = lax.broadcasted_iota(jnp.int32, (32, CHOSEN), 1).astype(F32)
        rank = lax.broadcasted_iota(jnp.int32, (32, 1), 0).astype(F32)
        hit = lane == rank + (shift + (i * 32).astype(F32))
        spot = jnp.sum(jnp.where(hit, spots_f[...], 0.0), axis=1, keepdims=True)
        gate = jnp.sum(jnp.where(hit, grow[...], 0.0), axis=1, keepdims=True)
        cpos[0, rows, :] = jnp.broadcast_to(spot, (32, 128))
        cpos[1, rows, :] = jnp.broadcast_to(gate, (32, 128))
        return carry

    lax.fori_loop(0, MOST // 32, pick, 0)
    place = lax.broadcasted_iota(jnp.int32, (MOST, TOK), 1).astype(F32)
    onehot[...] = jnp.where(place == cpos[0, :, 0:1] - base, 1.0, 0.0).astype(BF16)

    for copy in loads:
        copy.wait()
    pl.semaphore_wait(barrier, SEQ + 2)

    z_places, x_places = places(NZ, NX), places(NX, NZ)
    z_blocks, x_blocks = list(z_places), list(x_places)

    def block_at(i):
        return zf(z_blocks[i])

    def q_copy(s, k, sem, to):
        piece = wqo.at[0, s, along_y(k)]
        return remote(piece, piece, q_send, q_recv.at[sem], along_y(to), me)

    def to_y(n):
        s = block_at(n)
        q_copy(s, 0, n // 2, 1).start()
        q_copy(s, 0, n // 2, -1).start()
        q_across(s, 0)

    def q_across(s, k):
        piece = wqo.at[0, s, along_y(k)]
        remote(piece, piece, p_send, p_recv.at[0], partner, me).start()

    def from_y(i):
        both = wqo.at[0, pl.ds(0, 4), 0]
        pltpu.make_async_copy(both, both, q_recv.at[i]).wait()
        low, high = block_at(2 * i), block_at(2 * i + 1)
        q_copy(low, -1, SEQ // 2, 1).start()
        q_copy(high, 1, SEQ // 2, -1).start()
        for s in (low, high):
            q_across(s, -1)
            q_across(s, 1)

    def first_gather(far, view, many, send_sem, recv_sem, arrived):
        groups = ring_groups(NZ, NX)[0]

        def send(block, to):
            group = z_places[(block[0] - to[0]) % NZ, (block[1] - to[1]) % NX][1]
            s = zf(block)
            remote(view(s), view(s), send_sem, recv_sem.at[group], dp, zf(to)).start()

        def wait(index):
            some = many(len(groups[index]))
            pltpu.make_async_copy(some, some, recv_sem.at[index]).wait()

        def then(index, step):
            step()
            for block in groups[index]:
                arrived(z_places[block[0] % NZ, block[1] % NX][0])

        steps = ring_steps(NZ, NX, True, far, send, wait)
        return [functools.partial(then, index, step) for index, step in enumerate(steps)]

    def kv_half(s):
        return kvw.at[kv_unit(s, core), :]

    def to_partner(n):
        half = kv_half(block_at(n))
        remote(half, half, d_send, d_recv, partner, me).start()

    w_steps = first_gather(
        False,
        kv_half, lambda n: kvw.at[pl.ds(0, n * HALF), :], w_send, w_recv, to_partner,
    )
    q_steps = first_gather(
        True,
        lambda s: wqo.at[0, s, dp], lambda n: wqo.at[0, pl.ds(0, n), 0],
        o_send.at[0], o_recv.at[0], to_y,
    )
    o_steps = first_gather(
        True,
        lambda s: wqo.at[1, s, dp], lambda n: wqo.at[1, pl.ds(0, n), 0],
        o_send.at[1], o_recv.at[1], lambda n: None,
    )

    def gather_rows(n):
        columns = slice(n * 256, (n + 1) * 256)
        part = jnp.dot(onehot[...], tok[:, columns], preferred_element_type=F32)
        normed[:, columns] = part.astype(BF16)
        square = jnp.broadcast_to(jnp.sum(part * part, axis=1, keepdims=True), (MOST, 128))
        wide[...] = square if n == 0 else wide[...] + square

    def normalize(n):
        columns = slice(n * 512, (n + 1) * 512)
        scale = lax.rsqrt(wide[:, 0:1] * (1.0 / D) + 1e-06)
        normed[:, columns] = (normed[:, columns].astype(F32) * scale).astype(BF16)

    def place_rows():
        order = lax.broadcasted_iota(jnp.int32, (MOST, MOST), 1)
        slot = lax.broadcasted_iota(jnp.int32, (MOST, MOST), 0)
        rank = order + shift.astype(jnp.int32)
        offset = rank - first.astype(jnp.int32)
        inside = jnp.where(offset >= 0, 1, 0) * jnp.where(rank < last.astype(jnp.int32), 1, 0)
        goes = (rank & (SEQ - 1)) * SLOTS + (offset >> 5)
        deal[...] = jnp.where(goes == slot, inside, 0).astype(F32).astype(BF16)
        gate = cpos[1, :, 0:1]
        eye = order == slot
        meta[0:1, :] = jnp.sum(jnp.where(eye, cpos[0, :, 0:1] - base, 0.0), axis=0, keepdims=True)
        meta[1:2, :] = jnp.sum(jnp.where(eye, gate, 0.0), axis=0, keepdims=True)

    def dealt_order():
        rows = listed_in[...].astype(F32)
        r = lax.broadcasted_iota(jnp.int32, (SEQ, ROWS), 0)
        k = lax.broadcasted_iota(jnp.int32, (SEQ, ROWS), 1)
        for q in range(ROWS // SEQ):
            take_k = jnp.where(k == r * (ROWS // SEQ) + q, 1.0, 0.0)
            part = lax.dot_general(
                rows[:, q * SEQ : (q + 1) * SEQ], take_k, (((0,), (0,)), ((), ())),
                precision=lax.Precision.HIGHEST, preferred_element_type=F32,
            )
            c2t[...] = part if q == 0 else c2t[...] + part

    def find_slots():
        lane32 = lax.broadcasted_iota(jnp.int32, (ROWS, SEQ), 1)
        mine = jnp.sum(jnp.where(lane32 == me, c2t[...].T, 0.0), axis=1, keepdims=True)
        source = jnp.floor(mine * (1.0 / TOK))

        def before(i, total):
            columns = pl.ds(pl.multiple_of(i * 512, 512), 512)
            return total + jnp.sum(
                jnp.where(spots_f[:, columns] < source * TOK, 1.0, 0.0), axis=1, keepdims=True
            )

        starts = lax.fori_loop(0, CHOSEN // 512, before, jnp.zeros((ROWS, 1), F32))
        my_rank = lax.broadcasted_iota(jnp.int32, (ROWS, 1), 0).astype(F32) * SEQ + me.astype(F32)
        found = source * SLOTS + jnp.floor((my_rank - starts) * (1.0 / SEQ))
        take[...] = jnp.where(
            lax.broadcasted_iota(jnp.int32, (ROWS, MOST), 1).astype(F32) == found, 1.0, 0.0
        ).astype(BF16)

    def bias_blocks(low, high):
        for slot in range(low, high):
            spots = jnp.where(
                lax.broadcasted_iota(jnp.int32, (1, ROWS), 1) < SIDE,
                c2t[pl.ds(zf(z_blocks[slot]), 1), :],
                c2t[pl.ds(xf(x_blocks[slot]), 1), :],
            )
            bias[:, slot * ROWS : (slot + 1) * ROWS] = jnp.where(
                spots <= cpos[0, :, 0:1], 0.0, FAR
            )

    work = [functools.partial(gather_rows, n) for n in range(D // 256)]
    work += [functools.partial(normalize, n) for n in range(D // 512)]
    work += [place_rows]

    w_steps[0]()
    token_load.wait()
    done = 0
    for i in range(1, len(w_steps)):
        until = len(work) * i // (len(w_steps) - 1)
        for item in work[done:until]:
            item()
        done = until
        w_steps[i]()
        if i == NZ - 1:
            q_steps[0]()
            o_steps[0]()

    for n in range(1, NZ):
        q_steps[n]()
    for n in range(1, NZ):
        o_steps[n]()

    def part(a, k, low=0, high=SEQ):
        return wqo.at[a, pl.ds(low, high - low), along_y(k)]

    def along(a, k, slot, to, low=0, high=SEQ):
        return remote(
            part(a, k, low, high), part(a, k, low, high), y_send, y_recv.at[a, slot], along_y(to), me
        )

    def across(a, k):
        remote(part(a, k), part(a, k), p_send, p_recv.at[a], partner, me).start()

    def y_first(a):
        along(a, 0, 0, 1).start()
        along(a, 0, 1, -1).start()
        across(a, 0)

    def y_second(a):
        along(a, -1, 0, 1).wait_recv()
        along(a, -1, 2, 1, 0, SEQ // 2).start()
        across(a, -1)
        along(a, 1, 1, -1).wait_recv()
        along(a, 1, 3, -1, SEQ // 2, SEQ).start()
        across(a, 1)

    def y_third(a):
        along(a, 2, 2, 1, 0, SEQ // 2).wait_recv()
        along(a, 2, 3, -1, SEQ // 2, SEQ).wait_recv()
        across(a, 2)

    def y_last(a):
        whole = wqo.at[a, :, pl.ds(0, 4)]
        pltpu.make_async_copy(whole, whole, p_recv.at[a]).wait()

    whole = kvw.at[pl.ds(0, HALF * SEQ), :]
    pltpu.make_async_copy(whole, whole, d_recv).wait()

    for n in range(2):
        columns = slice(n * 256, (n + 1) * 256)
        kv_own[:, columns] = jnp.dot(
            normed[...], kvw[:, columns], preferred_element_type=F32
        ).astype(BF16)
    leaving = jnp.dot(deal[...], kv_own[...], preferred_element_type=F32)
    kv_slots[...] = leaving.reshape(SEQ, SLOTS, 2 * KW).astype(BF16)

    def send_slot(j, carry):
        dest = lax.rem(me + j, SEQ)
        remote(kv_slots.at[dest], kv_in.at[me], a_send, a_recv, dp, dest).start()
        return carry

    lax.fori_loop(1, SEQ, send_slot, 0)
    kv_in[me] = kv_slots[me]

    for i in range(NZ, len(q_steps)):
        q_steps[i]()
    dealt_order()
    find_slots()
    for n in range(8):
        bias_blocks(4 * n, 4 * n + 4)
        if n < EARLY:
            from_y(n)

    whole = kv_in.at[pl.ds(0, SEQ - 1)]
    pltpu.make_async_copy(whole, whole, a_recv).wait()
    came = kv_in[...].astype(F32).reshape(MOST, 2 * KW).astype(BF16)
    kv[0:ROWS, :] = jnp.dot(take[...], came, preferred_element_type=F32).astype(BF16)

    def second_gather(route, at, na, nb, order):
        groups = ring_groups(na, nb)[0]

        def rows(n):
            return kv.at[pl.ds(n * ROWS + route * SIDE, SIDE), :]

        def send(block, to):
            n = order[block[0] % na, block[1] % nb][0]
            lands, group = order[(block[0] - to[0]) % na, (block[1] - to[1]) % nb]
            remote(rows(n), rows(lands), kv_send, kv_recv.at[route, group], dp, at(to)).start()

        def wait(index):
            some = kv.at[pl.ds(0, len(groups[index]) * SIDE), :]
            pltpu.make_async_copy(some, some, kv_recv.at[route, index]).wait()

        return ring_steps(na, nb, False, False, send, wait)

    z_steps = second_gather(0, zf, NZ, NX, z_places)
    x_steps = second_gather(1, xf, NX, NZ, x_places)

    def attend(g, pair):
        e = pair // (GROUP // PAIR)
        rows = slice(g * CHUNK, (g + 1) * CHUNK)
        keys = kv[rows, pl.ds(pl.multiple_of(e * HEAD_DIM, HEAD_DIM), HEAD_DIM)]
        values = kv[rows, pl.ds(pl.multiple_of(KW + e * HEAD_DIM, HEAD_DIM), HEAD_DIM)]
        heads = [pair * PAIR + n for n in range(PAIR)]
        columns = [pl.ds(pl.multiple_of(h * HEAD_DIM, HEAD_DIM), HEAD_DIM) for h in heads]
        scores = [
            lax.dot_general(
                query[:, c], keys, (((1,), (1,)), ((), ())), preferred_element_type=F32
            )
            for c in columns
        ]
        for h, c, score in zip(heads, columns, scores):
            score = score + bias[:, rows]
            fresh = jnp.max(score, axis=1, keepdims=True)
            if g > 0:
                before = top_ref[h][:, 0:1]
                fresh = jnp.maximum(before, fresh)
            probs = jnp.exp(score - fresh)
            total = jnp.sum(probs, axis=1, keepdims=True)
            acc = jnp.dot(probs.astype(BF16), values, preferred_element_type=F32)
            if g > 0:
                shrink = jnp.exp(before - fresh)
                total = total_ref[h][:, 0:1] * shrink + total
                acc = acc_ref[h] * shrink + acc
            if g < CHOSEN // CHUNK - 1:
                top_ref[h] = jnp.broadcast_to(fresh, (MOST, 128))
                total_ref[h] = jnp.broadcast_to(total, (MOST, 128))
                acc_ref[h] = acc
            else:
                att[:, c] = (acc / total).astype(BF16)

    def project_q():
        def tile(n, carry):
            columns = pl.ds(pl.multiple_of(n * 256, 256), 256)
            weights = wqo[0, :, :, :, columns].reshape(D, 256)
            piece = jnp.dot(normed[...], weights, preferred_element_type=F32)
            query[:, columns] = (piece * HEAD_DIM ** (-0.5)).astype(BF16)
            return carry

        lax.fori_loop(0, QW // 256, tile, 0)

    def last_of_y():
        y_first(1)
        whole = wqo.at[0, :, 0]
        pltpu.make_async_copy(whole, whole, q_recv.at[SEQ // 2]).wait()
        across(0, 2)

    z_steps[0]()
    x_steps[0]()
    for i in range(EARLY, SEQ // 2):
        from_y(i)
        if i == 9:
            z_steps[1]()
            x_steps[1]()
            z_steps[2]()
            x_steps[2]()
        if i == 14:
            x_steps[3]()
            z_steps[3]()
            z_steps[4]()
    for i in range(NZ, len(o_steps)):
        o_steps[i]()
    x_steps[4]()
    z_steps[5]()
    z_steps[6]()
    last_of_y()
    x_steps[5]()
    y_last(0)
    project_q()
    z_steps[7]()

    windows = {
        1: [[z_steps[n + 8], x_steps[n + 6]] for n in range(4)],
        2: [[z_steps[n + 12], x_steps[n + 10]] for n in range(4)],
        3: [[x_steps[14]], [x_steps[15]], [z_steps[16]], [x_steps[16]]],
    }
    windows = {g: [w[0] + w[1], w[2] + w[3]] for g, w in windows.items()}
    for g in range(1, CHOSEN // CHUNK):
        if g == 3:
            y_second(1)

        def together(i, carry):
            for j in range(HEADS // PAIR):

                @pl.when(i == j)
                def _():
                    for step in windows[g][j]:
                        step()

            attend(g - 1, i)
            return carry

        lax.fori_loop(0, HEADS // PAIR, together, 0)

    def alone(i, carry):
        attend(CHOSEN // CHUNK - 1, i)
        return carry

    lax.fori_loop(0, HEADS // PAIR, alone, 0)
    y_third(1)
    y_last(1)

    def project_out(n, carry):
        columns = pl.ds(pl.multiple_of(n * 256, 256), 256)
        weights = wqo[1, pl.ds(n * 4, 4)].reshape(256, QW)
        out_tile[n] = lax.dot_general(
            att[...], weights, (((1,), (1,)), ((), ())), preferred_element_type=F32
        ).astype(BF16)
        pltpu.make_async_copy(out_tile.at[n], out.at[n], out_sem.at[0]).start()
        return carry

    meta_copy = pltpu.make_async_copy(meta, meta_out, out_sem.at[1])
    meta_copy.start()
    lax.fori_loop(0, D // 256, project_out, 0)

    for whole, sem in (
        (kvw.at[pl.ds(0, HALF * (SEQ - 1)), :], w_send),
        (kvw.at[pl.ds(0, HALF * SEQ), :], d_send),
        (wqo.at[0, pl.ds(0, SEQ - 1), 0], o_send.at[0]),
        (wqo.at[1, pl.ds(0, SEQ - 1), 0], o_send.at[1]),
        (kv_in.at[pl.ds(0, SEQ - 1)], a_send),
        (kv.at[pl.ds(0, ROWS * (SEQ - 1)), :], kv_send),
        (wqo.at[0, :, pl.ds(0, 3)], q_send),
        (wqo.at[1, :, pl.ds(0, 3)], y_send),
        (wqo.at[:, :, pl.ds(0, 4)], p_send),
    ):
        pltpu.make_async_copy(whole, whole, sem).wait()
    meta_copy.wait()
    pltpu.make_async_copy(out_tile, out, out_sem.at[0]).wait()


def mix_kernel(tokens, block_out, meta, mixed, tok, rows_in, result, load_sem, rows_sem, store_sem):
    def load(n):
        return pltpu.make_async_copy(tokens.at[n], tok.at[n], load_sem.at[n])

    def store(n, half):
        columns = slice(half * 1024, (half + 1) * 1024)
        return pltpu.make_async_copy(
            result.at[n, :, columns], mixed.at[n, :, columns], store_sem.at[half, n]
        )

    rows_load = pltpu.make_async_copy(block_out, rows_in, rows_sem)
    rows_load.start()
    for n in range(TILES):
        load(n).start()
    rows_load.wait()

    def tile(n, carry):
        place = lax.broadcasted_iota(jnp.int32, (TILE, MOST), 0) + n * TILE
        hit = place.astype(F32) == meta[0:1, :]
        gate = jnp.sum(jnp.where(hit, meta[1:2, :], 0.0), axis=1, keepdims=True)
        gate = jnp.broadcast_to(gate, (TILE, 256))
        chosen_row = jnp.where(hit, 1.0, 0.0).astype(BF16)
        load(n).wait()
        for c in range(D // 256):
            columns = slice(c * 256, (c + 1) * 256)
            rows = jnp.dot(chosen_row, rows_in[c], preferred_element_type=F32)
            result[n, :, columns] = (tok[n, :, columns].astype(F32) + gate * rows).astype(BF16)
            if c % 4 == 3:
                store(n, c // 4).start()
        return carry

    lax.fori_loop(0, TILES, tile, 0)
    for n in range(TILES):
        for half in range(2):
            store(n, half).wait()


def per_device(tokens, chosen, gates, w_query, w_key, w_value, w_out):
    anywhere = pl.BlockSpec(memory_space=pl.ANY)
    inside = pl.BlockSpec(memory_space=pltpu.VMEM)
    dma = pltpu.SemaphoreType.DMA
    vmem = pltpu.VMEM
    block_out, meta = pl.pallas_call(
        block_kernel,
        out_shape=(
            jax.ShapeDtypeStruct((D // 256, MOST, 256), BF16),
            jax.ShapeDtypeStruct((8, MOST), F32),
        ),
        in_specs=[anywhere] * 5 + [inside] * 3,
        out_specs=(anywhere, anywhere),
        scratch_shapes=[
            vmem((D // 256, MOST, 256), BF16),
            vmem((8, MOST), F32),
            vmem((TOK, D), BF16),
            vmem((D, 2 * KW), BF16),
            vmem((2, SEQ, PARTS, PIECE, QW), BF16),
            vmem((MOST, D), BF16),
            vmem((MOST, TOK), BF16),
            vmem((MOST, MOST), BF16),
            vmem((ROWS, MOST), BF16),
            vmem((MOST, CHOSEN), F32),
            vmem((MOST, QW), BF16),
            vmem((MOST, QW), BF16),
            vmem((MOST, 2 * KW), BF16),
            vmem((SEQ, SLOTS, 2 * KW), BF16),
            vmem((SEQ, SLOTS, 2 * KW), BF16),
            vmem((CHOSEN, 2 * KW), BF16),
            vmem((2, MOST, 128), F32),
            vmem((1, CHOSEN), F32),
            vmem((SEQ, ROWS), F32),
            vmem((MOST, 128), F32),
            vmem((HEADS, MOST, 128), F32),
            vmem((HEADS, MOST, 128), F32),
            vmem((HEADS, MOST, 128), F32),
            dma((4,)),
            dma,
            dma((2,)),
            dma,
            dma((17,)),
            dma((2,)),
            dma((2, 17)),
            dma,
            dma,
            dma,
            dma,
            dma,
            dma((2, 17)),
            dma,
            dma((17,)),
            dma,
            dma((2, 4)),
            dma,
            dma((2,)),
        ],
        compiler_params=pltpu.CompilerParams(
            collective_id=0, has_side_effects=True, vmem_limit_bytes=56 * 1024 * 1024
        ),
        name="block",
    )(
        tokens,
        w_query.reshape(PARTS, PIECE, QW),
        w_key,
        w_value,
        w_out.T.reshape(PARTS, PIECE, QW),
        chosen.reshape(1, CHOSEN),
        gates.reshape(1, CHOSEN),
        chosen.reshape(SEQ, ROWS),
    )
    mixed = pl.pallas_call(
        mix_kernel,
        out_shape=jax.ShapeDtypeStruct((TILES, TILE, D), BF16),
        in_specs=[anywhere, anywhere, inside],
        out_specs=anywhere,
        scratch_shapes=[
            vmem((TILES, TILE, D), BF16),
            vmem((D // 256, MOST, 256), BF16),
            vmem((TILES, TILE, D), BF16),
            dma((TILES,)),
            dma,
            dma((2, TILES)),
        ],
        compiler_params=pltpu.CompilerParams(vmem_limit_bytes=56 * 1024 * 1024),
        name="mix",
    )(tokens.reshape(TILES, TILE, D), block_out, meta)
    return mixed.reshape(TOK, D)


def solution(mesh):
    return jax.shard_map(
        per_device,
        mesh=mesh,
        in_specs=(
            P(("dp", "seq"), None),
            P("dp"),
            P("dp"),
            P("seq", None),
            P("seq", None),
            P("seq", None),
            P(None, "seq"),
        ),
        out_specs=P(("dp", "seq"), None),
        check_vma=False,
    )
```
